256 devices in a mesh: section: 16 (over z, core), board: 16 (over y, x).
Axes of the slice: x: 4, y: 4, z: 8, core: 2. Of those that a mesh axis runs over, the one named last changes fastest.
Arguments:
- root_reach: float32 [2, 8, 1326], replicated, may hold values from 0.05 to 1
- frontier_value: float32 [2, 8, 1326], replicated, may hold values from -60 to 60
- regret_stop: float32 [16, 64, 8, 1326], P('section', 'board'), may hold values from 1 to 30
- regret_go: float32 [16, 64, 8, 1326], P('section', 'board'), may hold values from 1 to 30
- board_live: int32 [64], P('board'), may hold values from 0 to 1, as said below
- board_cards: int32 [64, 5], P('board'), may hold values from 0 to 51, as said below
- hand_rank: int32 [64, 1326], P('board'), may hold values from 0 to 1325
Outputs:
- new_stop: float32 [16, 64, 8, 1326], P('section', 'board')
- new_go: float32 [16, 64, 8, 1326], P('section', 'board')
- section_values: float32 [16, 2, 8, 1326], P('section')
The draws below stay inside these ranges and needn't reach their ends.
Inputs may be any that keep to these rules, and one draw needn't show every extreme that they name: `board_live`: 0 or 1; among each device's 4 slots the first one is always 1. `board_cards`: a slot's 5 cards are distinct. `hand_rank`: equal values tie.
All inputs are finite; a program needn't handle non-finite values.
Results may differ from the reference program's by a relative error of at most 0.0008.
Values sent between devices are 32-bit elements; how exact they have to be, the bound alone decides.
A program may use at most 64 MiB of HBM per device.

```python
import math
import jax
import jax.numpy as jnp
import numpy as np
from jax import lax

CARDS = 52
BOARD_CARDS = 5
H = 1326
NODES = 8
BOARD_DEV = 4
SLOTS = 64
SECTIONS = 16


def draw_board_cards(key, part):
    keys = jax.random.split(jax.random.fold_in(key, 17), SLOTS)

    def one_board(board_key):
        return jax.random.permutation(board_key, CARDS)[:BOARD_CARDS].astype(jnp.int32)
    return jax.vmap(one_board)(keys)


def draw_board_live(key, part):
    coins = jax.random.randint(jax.random.fold_in(key, 29), (SLOTS,), 0, 2).astype(jnp.int32)
    leading = jnp.arange(SLOTS) % BOARD_DEV == 0
    return jnp.where(leading, 1, coins).astype(jnp.int32)


def place_ends(drawn, key, low, top_value):
    index_at = [jax.random.randint(jax.random.fold_in(key, axis), (), 0, length) for axis, length in enumerate(drawn.shape)]
    main_axis = drawn.shape.index(max(drawn.shape))
    next_to = index_at[:main_axis] + [(index_at[main_axis] + 1) % drawn.shape[main_axis]] + index_at[main_axis + 1:]
    return drawn.at[tuple(index_at)].set(low).at[tuple(next_to)].set(top_value)


def level_of(own_key, dims, shards, low, largest):
    loudness = 1.0
    for position, shards_of in shards:
        steps = jax.random.uniform(jax.random.fold_in(jax.random.fold_in(own_key, 6), position), (shards_of,), jnp.float32, low / len(shards), largest / len(shards))
        loudness = loudness * jnp.repeat(jnp.exp(steps), dims[position] // shards_of).reshape((-1,) + (1,) * (len(dims) - 1 - position))
    return loudness


def scatter_about(stream_key, dims, width, most, kind=jnp.bfloat16):
    values = jax.random.normal(stream_key, dims, jnp.float32) * width
    return jnp.minimum(jnp.maximum(values, -most), most).astype(kind)


def setup_inputs(seed: int = 0) -> dict:
    seeds = jax.random.split(jax.random.key(seed), 8)
    return {
        "root_reach": jnp.clip(jnp.exp(jax.random.uniform(seeds[0], (2, NODES, H), jnp.float32, math.log(0.05), math.log(1.0))), 0.05, 1.0),
        "frontier_value": scatter_about(seeds[1], (2, NODES, H), 10.0, 60.0, jnp.float32),
        "regret_stop": jnp.clip(jnp.exp(math.log(30.0) - 3.4011974 * jax.random.uniform(seeds[2], (SECTIONS, SLOTS, NODES, H), jnp.float32) ** level_of(seeds[2], (SECTIONS, SLOTS, NODES, H), ((0, 16), (1, 16)), -0.2, 0.2)), 1.0, 30.0),
        "regret_go": jnp.clip(jnp.exp(math.log(30.0) - 3.4011974 * jax.random.uniform(seeds[3], (SECTIONS, SLOTS, NODES, H), jnp.float32) ** level_of(seeds[3], (SECTIONS, SLOTS, NODES, H), ((0, 16), (1, 16)), -0.2, 0.2)), 1.0, 30.0),
        "board_live": draw_board_live(jax.random.fold_in(seeds[7], 71), 0),
        "board_cards": draw_board_cards(jax.random.fold_in(seeds[7], 71), 0),
        "hand_rank": place_ends(jax.random.randint(seeds[6], (SLOTS, H), 0, H), jax.random.fold_in(seeds[6], 1), 0, H - 1).astype(jnp.int32),
    }


def free_pairs():
    first, second = np.triu_indices(CARDS, 1)
    first = jnp.asarray(first.astype(np.int32))
    second = jnp.asarray(second.astype(np.int32))
    shared = (first[:, None] == first[None, :]) | (first[:, None] == second[None, :]) | (second[:, None] == first[None, :]) | (second[:, None] == second[None, :])
    return jnp.where(shared, 0.0, 1.0).astype(jnp.bfloat16)


def board_masks(board_cards):
    first, second = np.triu_indices(CARDS, 1)
    first = jnp.asarray(first.astype(np.int32))
    second = jnp.asarray(second.astype(np.int32))
    hits = (board_cards[:, :, None] == first[None, None, :]) | (board_cards[:, :, None] == second[None, None, :])
    return jnp.where(jnp.any(hits, axis=1), 0.0, 1.0).astype(jnp.float32)


def showdown(reach_one, stop_weight, mask_row, rank_row, disjoint):
    leaf_reach = (reach_one * stop_weight).astype(jnp.bfloat16)
    mask_half = mask_row.astype(jnp.bfloat16)
    payoff = jnp.sign(rank_row[:, None] - rank_row[None, :]).astype(jnp.bfloat16) * disjoint * mask_half[:, None] * mask_half[None, :]
    flipped = leaf_reach[::-1].reshape(-1, leaf_reach.shape[-1])
    result = jnp.dot(flipped.astype(jnp.float32), payoff.astype(jnp.float32).T, precision=lax.Precision.HIGHEST)
    return result.reshape(leaf_reach.shape)


def reference(root_reach, frontier_value, regret_stop, regret_go, board_live, board_cards, hand_rank):
    disjoint = free_pairs()
    masks = board_masks(board_cards)
    regret_sum = regret_stop + regret_go
    stop_prob = regret_stop / regret_sum
    go_prob = regret_go / regret_sum
    alive = (board_live > 0).astype(jnp.float32)
    board_total = jnp.sum(alive)
    depth_total = regret_stop.shape[0]
    players = jnp.arange(2)[:, None, None]
    reach_now = root_reach[None] * masks[:, None, None, :]
    leaf_store = []
    for level in range(depth_total):
        acting = players == level % 2
        factor = jnp.where(acting[None], go_prob[level][:, None], 1.0)
        stop_weight = jnp.where(acting[None], stop_prob[level][:, None], 1.0)

        def one_board(items):
            reach_one, weight_one, mask_row, rank_row, alive_one = items
            return lax.cond(alive_one > 0,
                            lambda: showdown(reach_one, weight_one, mask_row, rank_row, disjoint),
                            lambda: jnp.zeros(reach_one.shape, jnp.float32))

        leaf_values = lax.map(one_board, (reach_now, stop_weight, masks, hand_rank, alive))
        leaf_store.append(leaf_values)
        reach_now = reach_now * factor
    value_next = frontier_value[None] * masks[:, None, None, :]
    nexts = [None] * depth_total
    totals = [None] * depth_total
    for level in reversed(range(depth_total)):
        acting = players == level % 2
        factor = jnp.where(acting[None], go_prob[level][:, None], 1.0)
        stop_weight = jnp.where(acting[None], stop_prob[level][:, None], 1.0)
        nexts[level] = value_next
        value_next = stop_weight * leaf_store[level] + factor * value_next
        totals[level] = jnp.sum(alive[:, None, None, None] * value_next, axis=0) / board_total
    stops = []
    goes = []
    for level in range(depth_total):
        acting = players == level % 2
        own_next = jnp.sum(jnp.where(acting[None], nexts[level], 0.0), axis=1)
        own_leaf = jnp.sum(jnp.where(acting[None], leaf_store[level], 0.0), axis=1)
        gap = own_leaf - own_next
        keep_slot = alive[:, None, None] > 0
        stops.append(jnp.where(keep_slot, jnp.maximum(regret_stop[level] + go_prob[level] * gap, 0.0), regret_stop[level]))
        goes.append(jnp.where(keep_slot, jnp.maximum(regret_go[level] - stop_prob[level] * gap, 0.0), regret_go[level]))
    return (jnp.stack(stops), jnp.stack(goes), jnp.stack(totals))
```

```python
import jax
import jax.numpy as jnp
import numpy as np
from jax import lax
from jax.experimental import pallas as pl
from jax.experimental.pallas import tpu as pltpu
from jax.sharding import PartitionSpec as P

CARDS = 52
H = 1326
NODES = 8
TILES = 11
HP = TILES * 128
LAST = H - 128 * (TILES - 1)
SECTIONS = 16
COLUMNS = 16
BOARD_DEV = 4
ROWS = 24
HALF = 16
MESH = pl.DeviceIdType.MESH


def hand_bits():
    first, second = np.triu_indices(CARDS, 1)
    low = np.full((HP,), -1, np.int64)
    high = np.full((HP,), -1, np.int64)
    both = (np.int64(1) << first) | (np.int64(1) << second)
    low[:H] = both & 0xFFFFFFFF
    high[:H] = both >> 32
    rows = np.stack([low, high]).astype(np.uint32).view(np.int32)
    scan = np.full((2, ROWS, 128), -1, np.int32)
    for word in range(2):
        tiles = rows[word].reshape(TILES, 128)
        scan[word, :TILES] = tiles
        scan[word, TILES : 2 * TILES] = tiles
    return rows, scan.reshape(2 * ROWS, 128)


def remote(src, dst, send, recv, section, board):
    return pltpu.make_async_remote_copy(
        src_ref=src,
        dst_ref=dst,
        send_sem=send,
        recv_sem=recv,
        device_id={"section": section, "board": board},
        device_id_type=MESH,
    )


def slot(ref, index, rows):
    return ref.at[pl.ds(pl.multiple_of(index * rows, 8), rows), :]


def kernel(
    root_hbm, front_hbm, stop_hbm, go_hbm, live_hbm, cards_hbm, rank_hbm, bits_hbm, scan_hbm,
    out_stop, out_go, out_sec,
    root_v, front_v, stop_v, go_v, live_s, cards_s, rank_v, bits_v, scan_v,
    pad, asend, arecv, ends, colrow, cols, bcast, w, lsc, lhs, leafsc,
    gsend, grecv, nsc, rsend, rrecv, fsend, frecv,
    in_sem, a_ss, a_rs, g_ss, g_rs, r_ss, r_rs, f_ss, f_rs,
):
    me = lax.axis_index("section")
    col = lax.axis_index("board")
    node = me // 2
    core = me % 2

    barrier = pltpu.get_barrier_semaphore()
    for d in range(1, SECTIONS):
        pl.semaphore_signal(
            barrier, inc=1, device_id={"section": (me + d) % SECTIONS, "board": col}, device_id_type=MESH
        )
    for dc in range(2):
        for db in range(1, COLUMNS):
            pl.semaphore_signal(
                barrier,
                inc=1,
                device_id={"section": 2 * node + (core + dc) % 2, "board": (col + db) % COLUMNS},
                device_id_type=MESH,
            )

    loads = [
        pltpu.make_async_copy(src, dst, in_sem.at[i])
        for i, (src, dst) in enumerate(
            [
                (stop_hbm, stop_v), (go_hbm, go_v), (root_hbm, root_v), (front_hbm, front_v),
                (live_hbm, live_s), (cards_hbm, cards_s), (rank_hbm, rank_v), (bits_hbm, bits_v),
                (scan_hbm, scan_v),
            ]
        )
    ]
    for copy in loads:
        copy.start()
    pad[...] = jnp.full(pad.shape, 0.5, jnp.float32)
    ends[...] = jnp.zeros(ends.shape, jnp.float32)
    loads[0].wait()
    loads[1].wait()

    for j in range(BOARD_DEV):
        for t in range(TILES):
            if t < TILES - 1:
                at = pl.ds(128 * t, 128)
                tile = go_v[j, :, at] / (go_v[j, :, at] + stop_v[j, :, at])
            else:
                at = pl.ds(128 * t, LAST)
                pad[j, :, :LAST] = go_v[j, :, at] / (go_v[j, :, at] + stop_v[j, :, at])
                tile = pad[j]
            row = (j // 2) * ROWS + (j % 2) * TILES + t
            asend[pl.ds(row, NODES, stride=2 * ROWS), :] = tile
    pl.semaphore_wait(barrier, SECTIONS - 1 + 2 * (COLUMNS - 1))

    def a_copy(to):
        return remote(
            slot(asend, to, ROWS), slot(arecv, me, ROWS), a_ss.at[to], a_rs.at[me], to, col
        )

    order = sorted(range(1, SECTIONS), key=lambda d: -min(d, SECTIONS - d))
    for d in order:
        a_copy((me + d) % SECTIONS).start()
    own = pl.ds(pl.multiple_of(me * ROWS, 8), ROWS)
    arecv[own, :] = asend[own, :]

    for copy in loads[2:]:
        copy.wait()

    alive = []
    board_bits = []
    for jj in range(2):
        j = 2 * core + jj
        alive.append(jnp.where(live_s[j] > 0, 1.0, 0.0).astype(jnp.float32))
        low = jnp.int32(0)
        high = jnp.int32(0)
        for i in range(5):
            card = cards_s[j, i]
            bit = lax.shift_left(jnp.int32(1), card % 32)
            low = low | jnp.where(card < 32, bit, 0)
            high = high | jnp.where(card < 32, 0, bit)
        board_bits.append((low, high))
    row_id = lax.broadcasted_iota(jnp.int32, (ROWS, 128), 0)
    first_slot = row_id < TILES
    low = jnp.where(first_slot, board_bits[0][0], board_bits[1][0])
    high = jnp.where(first_slot, board_bits[0][1], board_bits[1][1])
    hit = (scan_v[:ROWS, :] & low) | (scan_v[ROWS:, :] & high)
    mask = jnp.where(hit == 0, 1.0, 0.0).astype(jnp.float32)
    inside = (scan_v[:ROWS, :] & scan_v[ROWS:, :]) != -1
    alive_rows = jnp.where(first_slot, alive[0], alive[1])

    for which, ref in enumerate((root_v, front_v)):
        for p in range(2):
            base = (2 * which + p) * NODES * ROWS
            pad[p, :, :] = jnp.zeros((NODES, 128), jnp.float32)
            pad[p, :, :LAST] = ref[p, :, pl.ds(128 * (TILES - 1), LAST)]
            for t in range(TILES):
                tile = ref[p, :, pl.ds(128 * t, 128)] if t < TILES - 1 else pad[p]
                ends[pl.ds(base + t, NODES, stride=ROWS), :] = tile
                ends[pl.ds(base + TILES + t, NODES, stride=ROWS), :] = tile

    def end_of(index):
        at = pl.multiple_of((index * NODES + node) * ROWS, 8)
        return jnp.where(mask > 0, ends[pl.ds(at, ROWS), :], 0.0)

    colrow[...] = jnp.zeros(colrow.shape, jnp.int32)
    colrow[0:2, :] = bits_v[...]
    for jj in range(2):
        colrow[2 + jj : 3 + jj, :H] = rank_v[pl.ds(2 * core + jj, 1), :]
    for r in range(4):
        bcast[r] = jnp.broadcast_to(colrow[r : r + 1, :], (8, HP))
    for t in range(TILES):
        cols[128 * t : 128 * (t + 1), :] = colrow[:, 128 * t : 128 * (t + 1)].T

    def payoff_rows(block, _):
        at = pl.multiple_of(block * 16, 16)
        col_of = cols[pl.ds(at, 16), :]
        wide = [jnp.broadcast_to(col_of[:, r : r + 1], (16, 128)) for r in range(4)]
        for t in range(TILES):
            lanes = slice(128 * t, 128 * (t + 1))
            row = [jnp.concatenate([bcast[r, :, lanes]] * 2, axis=0) for r in range(4)]
            free = ((wide[0] & row[0]) | (wide[1] & row[1])) == 0
            for jj in range(2):
                step = jnp.minimum(jnp.maximum(row[2 + jj] - wide[2 + jj], -1), 1)
                w[jj, pl.ds(at, 16), lanes] = jnp.where(free, step, 0).astype(jnp.float32).astype(jnp.bfloat16)
        return 0

    lax.fori_loop(0, HP // 16, payoff_rows, 0)

    for d in range(1, SECTIONS):
        other = (me + d) % SECTIONS
        remote(slot(asend, other, ROWS), slot(arecv, other, ROWS), a_ss.at[other], a_rs.at[other], other, col).wait_recv()

    reach = [end_of(0), end_of(1)]
    for s in range(SECTIONS):
        go = jnp.where(inside, arecv[s * ROWS : (s + 1) * ROWS, :], 0.5)
        q = s % 2
        lsc[q, s * ROWS : (s + 1) * ROWS, :] = reach[q] * (1.0 - go)
        lsc[1 - q, s * ROWS : (s + 1) * ROWS, :] = reach[1 - q]
        reach[q] = reach[q] * go
    for jj in range(2):
        for p in range(2):
            for t in range(TILES):
                tile = lsc[p, pl.ds(jj * TILES + t, SECTIONS, stride=ROWS), :]
                lhs[jj, p * SECTIONS : (p + 1) * SECTIONS, 128 * t : 128 * (t + 1)] = tile.astype(jnp.bfloat16)
    for jj in range(2):
        leaf = jnp.dot(lhs[jj], w[jj], preferred_element_type=jnp.float32)
        for p in range(2):
            for t in range(TILES):
                tile = leaf[p * SECTIONS : (p + 1) * SECTIONS, 128 * t : 128 * (t + 1)]
                leafsc[1 - p, pl.ds(jj * TILES + t, SECTIONS, stride=ROWS), :] = tile

    value = [end_of(2), end_of(3)]
    for s in reversed(range(SECTIONS)):
        q = s % 2
        rows = slice(s * ROWS, (s + 1) * ROWS)
        go = jnp.where(inside, arecv[rows, :], 0.5)
        leaf_q = leafsc[q, rows, :] * mask
        leaf_o = leafsc[1 - q, rows, :] * mask
        gsend[rows, :] = leaf_q - value[q]
        value[q] = (1.0 - go) * leaf_q + go * value[q]
        value[1 - q] = leaf_o + value[1 - q]
        for p in range(2):
            at = (2 * s + p) * ROWS
            nsc[at : at + ROWS, :] = jnp.where(inside, value[p], 1.0) * alive_rows
            half = (2 * s + p) * HALF
            rsend[half : half + TILES, :] = nsc[at : at + TILES, :] + nsc[at + TILES : at + 2 * TILES, :]

    def r_copy(dc, db):
        to_core = (core + dc) % 2
        to_col = (col + db) % COLUMNS
        to = 2 * node + to_core
        s = (to_col + to) % SECTIONS
        return remote(
            slot(rsend, 2 * s + to_core, HALF), rrecv.at[dc * COLUMNS + db], r_ss.at[dc * COLUMNS + db],
            r_rs.at[dc * COLUMNS + db], to, to_col,
        )

    pairs = [(dc, db) for db in range(COLUMNS) for dc in range(2) if dc or db]
    for dc, db in pairs:
        r_copy(dc, db).start()

    def g_copy(to):
        return remote(
            slot(gsend, to, ROWS), slot(grecv, me, ROWS), g_ss.at[to], g_rs.at[me], to, col
        )

    for d in order:
        g_copy((me + d) % SECTIONS).start()
    grecv[own, :] = gsend[own, :]

    mine = (col + me) % SECTIONS
    total = rsend[pl.ds(pl.multiple_of((2 * mine + core) * HALF, 8), HALF), :]
    for dc, db in pairs:
        r_copy(dc, db).wait_recv()
        total = total + rrecv[dc * COLUMNS + db]
    fsend[...] = total / total[TILES - 1 : TILES, 127:128]

    def f_copy(db):
        return remote(fsend, slot(frecv, me, HALF), f_ss.at[db], f_rs.at[me], mine, (col + db) % COLUMNS)

    for db in range(1, COLUMNS):
        f_copy(db).start()

    @pl.when(col != 0)
    def _():
        f_copy(0).start()

    @pl.when(col == 0)
    def _():
        frecv[pl.ds(pl.multiple_of(me * HALF, 8), HALF), :] = fsend[...]

    for d in range(1, SECTIONS):
        other = (me + d) % SECTIONS
        remote(slot(gsend, other, ROWS), slot(grecv, other, ROWS), g_ss.at[other], g_rs.at[other], other, col).wait_recv()
    for j in range(BOARD_DEV):
        keep = live_s[j] > 0
        for t in range(TILES):
            size = 128 if t < TILES - 1 else LAST
            at = pl.ds(128 * t, size)
            gap = grecv[pl.ds((j // 2) * ROWS + (j % 2) * TILES + t, NODES, stride=2 * ROWS), :][:, :size]
            stop = stop_v[j, :, at]
            go = go_v[j, :, at]
            total_regret = stop + go
            out_stop[j, :, at] = jnp.where(keep, jnp.maximum(stop + go / total_regret * gap, 0.0), stop)
            out_go[j, :, at] = jnp.where(keep, jnp.maximum(go - stop / total_regret * gap, 0.0), go)

    for k in range(SECTIONS):
        @pl.when(jnp.logical_or(me != k, col != 0))
        def _(k=k):
            remote(fsend, slot(frecv, k, HALF), f_ss.at[0], f_rs.at[k], mine, col).wait_recv()
    for p in range(2):
        for t in range(TILES):
            size = 128 if t < TILES - 1 else LAST
            tile = frecv[pl.ds(p * HALF + t, NODES, stride=2 * HALF), :]
            out_sec[p, :, pl.ds(128 * t, size)] = tile[:, :size]

    for d in order:
        a_copy((me + d) % SECTIONS).wait_send()
        g_copy((me + d) % SECTIONS).wait_send()
    for dc, db in pairs:
        r_copy(dc, db).wait_send()
    for db in range(1, COLUMNS):
        f_copy(db).wait_send()

    @pl.when(col != 0)
    def _():
        f_copy(0).wait_send()


def local(root_reach, frontier_value, regret_stop, regret_go, board_live, board_cards, hand_rank):
    bits, scan = hand_bits()
    f32, i32 = jnp.float32, jnp.int32
    regrets = (BOARD_DEV, NODES, H)
    ends = (2, NODES, H)
    any_spec = pl.BlockSpec(memory_space=pl.ANY)
    vmem_spec = pl.BlockSpec(memory_space=pltpu.VMEM)
    dma = pltpu.SemaphoreType.DMA
    new_stop, new_go, section_value = pl.pallas_call(
        kernel,
        out_shape=(
            jax.ShapeDtypeStruct(regrets, f32),
            jax.ShapeDtypeStruct(regrets, f32),
            jax.ShapeDtypeStruct(ends, f32),
        ),
        in_specs=[any_spec] * 9,
        out_specs=(vmem_spec,) * 3,
        scratch_shapes=[
            pltpu.VMEM(ends, f32), pltpu.VMEM(ends, f32), pltpu.VMEM(regrets, f32), pltpu.VMEM(regrets, f32),
            pltpu.SMEM((BOARD_DEV,), i32), pltpu.SMEM((BOARD_DEV, 5), i32), pltpu.VMEM((BOARD_DEV, H), i32),
            pltpu.VMEM((2, HP), i32), pltpu.VMEM((2 * ROWS, 128), i32),
            pltpu.VMEM((BOARD_DEV, NODES, 128), f32),
            pltpu.VMEM((SECTIONS * ROWS, 128), f32), pltpu.VMEM((SECTIONS * ROWS, 128), f32),
            pltpu.VMEM((4 * NODES * ROWS, 128), f32),
            pltpu.VMEM((8, HP), i32), pltpu.VMEM((HP, 8), i32), pltpu.VMEM((4, 8, HP), i32),
            pltpu.VMEM((2, HP, HP), jnp.bfloat16),
            pltpu.VMEM((2, SECTIONS * ROWS, 128), f32), pltpu.VMEM((2, 2 * SECTIONS, HP), jnp.bfloat16),
            pltpu.VMEM((2, SECTIONS * ROWS, 128), f32),
            pltpu.VMEM((SECTIONS * ROWS, 128), f32), pltpu.VMEM((SECTIONS * ROWS, 128), f32),
            pltpu.VMEM((2 * SECTIONS * ROWS, 128), f32),
            pltpu.VMEM((2 * SECTIONS * HALF, 128), f32), pltpu.VMEM((2 * COLUMNS, HALF, 128), f32),
            pltpu.VMEM((HALF, 128), f32), pltpu.VMEM((SECTIONS * HALF, 128), f32),
            dma((9,)), dma((SECTIONS,)), dma((SECTIONS,)), dma((SECTIONS,)), dma((SECTIONS,)),
            dma((2 * COLUMNS,)), dma((2 * COLUMNS,)), dma((COLUMNS,)), dma((SECTIONS,)),
        ],
        compiler_params=pltpu.CompilerParams(
            collective_id=0, has_side_effects=True, vmem_limit_bytes=40 * 1024 * 1024
        ),
    )(
        root_reach, frontier_value, regret_stop[0], regret_go[0], board_live, board_cards, hand_rank,
        jnp.asarray(bits), jnp.asarray(scan),
    )
    return new_stop[None], new_go[None], section_value[None]


def solution(mesh):
    regrets = P("section", "board", None, None)
    return jax.shard_map(
        local,
        mesh=mesh,
        in_specs=(P(), P(), regrets, regrets, P("board"), P("board", None), P("board", None)),
        out_specs=(regrets, regrets, P("section", None, None, None)),
        check_vma=False,
    )
```

```python
import jax
import jax.numpy as jnp
import numpy as np
from jax import lax
from jax.experimental import pallas as pl
from jax.experimental.pallas import tpu as pltpu
from jax.sharding import PartitionSpec as P

CARDS = 52
H = 1326
NODES = 8
TILES = 11
HP = TILES * 128
LAST = H - 128 * (TILES - 1)
SECTIONS = 16
COLUMNS = 16
BOARD_DEV = 4
ROWS = 24
BLOCK = 64
HALF = 16
MESH = pl.DeviceIdType.MESH


def hand_bits():
    first, second = np.triu_indices(CARDS, 1)
    low = np.full((HP,), -1, np.int64)
    high = np.full((HP,), -1, np.int64)
    both = (np.int64(1) << first) | (np.int64(1) << second)
    low[:H] = both & 0xFFFFFFFF
    high[:H] = both >> 32
    rows = np.stack([low, high]).astype(np.uint32).view(np.int32)
    scan = np.full((2, ROWS, 128), -1, np.int32)
    for word in range(2):
        tiles = rows[word].reshape(TILES, 128)
        scan[word, :TILES] = tiles
        scan[word, TILES : 2 * TILES] = tiles
    return rows, scan.reshape(2 * ROWS, 128)


def remote(src, dst, send, recv, section, board):
    return pltpu.make_async_remote_copy(
        src_ref=src,
        dst_ref=dst,
        send_sem=send,
        recv_sem=recv,
        device_id={"section": section, "board": board},
        device_id_type=MESH,
    )


def slot(ref, index, rows):
    used = 2 * TILES if rows == ROWS else TILES
    return ref.at[pl.ds(pl.multiple_of(index * rows, 8), used), :]


def kernel(
    root_hbm, front_hbm, stop_hbm, go_hbm, live_hbm, cards_hbm, rank_hbm, bits_hbm, scan_hbm,
    out_stop, out_go, out_sec,
    root_v, front_v, stop_v, go_v, live_s, cards_s, rank_v, bits_v, scan_v,
    pad, asend, arecv, ends, bitrow, rankrow, bitwide, rankwide, bitcol, rankcol, w, lsc, lhs, leafsc,
    gsend, grecv, nsc, rsend, rrecv, fsend, frecv,
    in_sem, a_ss, a_rs, g_ss, g_rs, r_ss, r_rs, f_ss, f_rs,
):
    me = lax.axis_index("section")
    col = lax.axis_index("board")
    node = me // 2
    core = me % 2

    barrier = pltpu.get_barrier_semaphore()
    for d in range(1, SECTIONS):
        pl.semaphore_signal(
            barrier, inc=1, device_id={"section": (me + d) % SECTIONS, "board": col}, device_id_type=MESH
        )
    for dc in range(2):
        for db in range(1, COLUMNS):
            pl.semaphore_signal(
                barrier,
                inc=1,
                device_id={"section": 2 * node + (core + dc) % 2, "board": (col + db) % COLUMNS},
                device_id_type=MESH,
            )

    loads = [
        pltpu.make_async_copy(src, dst, in_sem.at[i])
        for i, (src, dst) in enumerate(
            [
                (stop_hbm, stop_v), (go_hbm, go_v), (root_hbm, root_v), (front_hbm, front_v),
                (live_hbm, live_s), (cards_hbm, cards_s), (rank_hbm, rank_v), (bits_hbm, bits_v),
                (scan_hbm, scan_v),
            ]
        )
    ]
    for copy in loads:
        copy.start()
    pad[...] = jnp.full(pad.shape, 0.5, jnp.float32)
    ends[...] = jnp.zeros(ends.shape, jnp.float32)
    loads[0].wait()
    loads[1].wait()

    for j in range(BOARD_DEV):
        for t in range(TILES):
            if t < TILES - 1:
                at = pl.ds(128 * t, 128)
                tile = go_v[j, :, at] / (go_v[j, :, at] + stop_v[j, :, at])
            else:
                at = pl.ds(128 * t, LAST)
                pad[j, :, :LAST] = go_v[j, :, at] / (go_v[j, :, at] + stop_v[j, :, at])
                tile = pad[j]
            row = (j // 2) * ROWS + (j % 2) * TILES + t
            asend[pl.ds(row, NODES, stride=2 * ROWS), :] = tile
    pl.semaphore_wait(barrier, SECTIONS - 1 + 2 * (COLUMNS - 1))

    def a_copy(to):
        return remote(
            slot(asend, to, ROWS), slot(arecv, me, ROWS), a_ss.at[to], a_rs.at[me], to, col
        )

    order = sorted(range(1, SECTIONS), key=lambda d: -min(d, SECTIONS - d))
    for d in order:
        a_copy((me + d) % SECTIONS).start()
    own = pl.ds(pl.multiple_of(me * ROWS, 8), ROWS)
    arecv[own, :] = asend[own, :]

    for copy in loads[2:]:
        copy.wait()

    alive = []
    board_bits = []
    for jj in range(2):
        j = 2 * core + jj
        alive.append(jnp.where(live_s[j] > 0, 1.0, 0.0).astype(jnp.float32))
        low = jnp.int32(0)
        high = jnp.int32(0)
        for i in range(5):
            card = cards_s[j, i]
            bit = lax.shift_left(jnp.int32(1), card % 32)
            low = low | jnp.where(card < 32, bit, 0)
            high = high | jnp.where(card < 32, 0, bit)
        board_bits.append((low, high))
    row_id = lax.broadcasted_iota(jnp.int32, (ROWS, 128), 0)
    first_slot = row_id < TILES
    low = jnp.where(first_slot, board_bits[0][0], board_bits[1][0])
    high = jnp.where(first_slot, board_bits[0][1], board_bits[1][1])
    hit = (scan_v[:ROWS, :] & low) | (scan_v[ROWS:, :] & high)
    mask = jnp.where(hit == 0, 1.0, 0.0).astype(jnp.float32)
    inside = (scan_v[:ROWS, :] & scan_v[ROWS:, :]) != -1
    alive_rows = jnp.where(first_slot, alive[0], alive[1])

    for which, ref in enumerate((root_v, front_v)):
        for p in range(2):
            base = (2 * which + p) * NODES * ROWS
            pad[p, :, :] = jnp.zeros((NODES, 128), jnp.float32)
            pad[p, :, :LAST] = ref[p, :, pl.ds(128 * (TILES - 1), LAST)]
            for t in range(TILES):
                tile = ref[p, :, pl.ds(128 * t, 128)] if t < TILES - 1 else pad[p]
                ends[pl.ds(base + t, NODES, stride=ROWS), :] = tile
                ends[pl.ds(base + TILES + t, NODES, stride=ROWS), :] = tile

    def end_of(index):
        at = pl.multiple_of((index * NODES + node) * ROWS, 8)
        return jnp.where(mask > 0, ends[pl.ds(at, ROWS), :], 0.0)

    bitrow[...] = jnp.zeros(bitrow.shape, jnp.int32)
    bitrow[0:2, :] = bits_v[...]
    rankrow[...] = jnp.zeros(rankrow.shape, jnp.float32)
    for jj in range(2):
        rankrow[jj : jj + 1, :H] = rank_v[pl.ds(2 * core + jj, 1), :].astype(jnp.float32)
    for r in range(2):
        bitwide[r] = jnp.broadcast_to(bitrow[r : r + 1, :], (8, HP))
        rankwide[r] = jnp.broadcast_to(rankrow[r : r + 1, :], (8, HP))
    for t in range(TILES):
        lanes = slice(128 * t, 128 * (t + 1))
        bitcol[lanes, :] = bitrow[:, lanes].T
        rankcol[lanes, :] = rankrow[:, lanes].T

    def payoff_rows(block, _):
        at = [pl.multiple_of(block * BLOCK + 16 * i, 16) for i in range(BLOCK // 16)]
        wide = [
            [jnp.broadcast_to(ref[pl.ds(a, 16), r : r + 1], (16, 128)) for ref in (bitcol, rankcol) for r in range(2)]
            for a in at
        ]
        one = jnp.bfloat16(1)
        for t in range(TILES):
            lanes = slice(128 * t, 128 * (t + 1))
            low, high, rank0, rank1 = (
                jnp.concatenate([ref[r, :, lanes]] * 2, axis=0) for ref in (bitwide, rankwide) for r in range(2)
            )
            for a, (low_g, high_g, rank0_g, rank1_g) in zip(at, wide):
                shared = (low_g & low) | (high_g & high)
                free = jnp.where(shared == 0, 1.0, 0.0).astype(jnp.bfloat16)
                for jj, step in enumerate((rank0 - rank0_g, rank1 - rank1_g)):
                    step = step.astype(jnp.bfloat16)
                    w[jj, pl.ds(a, 16), lanes] = jnp.minimum(jnp.maximum(step, -one), one) * free
        return 0

    lax.fori_loop(0, HP // BLOCK, payoff_rows, 0)

    for d in range(1, SECTIONS):
        other = (me + d) % SECTIONS
        remote(slot(asend, other, ROWS), slot(arecv, other, ROWS), a_ss.at[other], a_rs.at[other], other, col).wait_recv()

    reach = [end_of(0), end_of(1)]
    for s in range(SECTIONS):
        go = jnp.where(inside, arecv[s * ROWS : (s + 1) * ROWS, :], 0.5)
        q = s % 2
        lsc[q, s * ROWS : (s + 1) * ROWS, :] = reach[q] * (1.0 - go)
        lsc[1 - q, s * ROWS : (s + 1) * ROWS, :] = reach[1 - q]
        reach[q] = reach[q] * go
    for jj in range(2):
        for p in range(2):
            for t in range(TILES):
                tile = lsc[p, pl.ds(jj * TILES + t, SECTIONS, stride=ROWS), :]
                lhs[jj, p * SECTIONS : (p + 1) * SECTIONS, 128 * t : 128 * (t + 1)] = tile.astype(jnp.bfloat16)
    for jj in range(2):
        leaf = jnp.dot(lhs[jj], w[jj], preferred_element_type=jnp.float32)
        for p in range(2):
            for t in range(TILES):
                tile = leaf[p * SECTIONS : (p + 1) * SECTIONS, 128 * t : 128 * (t + 1)]
                leafsc[1 - p, pl.ds(jj * TILES + t, SECTIONS, stride=ROWS), :] = tile

    value = [end_of(2), end_of(3)]
    for s in reversed(range(SECTIONS)):
        q = s % 2
        rows = slice(s * ROWS, (s + 1) * ROWS)
        go = jnp.where(inside, arecv[rows, :], 0.5)
        leaf_q = leafsc[q, rows, :] * mask
        leaf_o = leafsc[1 - q, rows, :] * mask
        gsend[rows, :] = leaf_q - value[q]
        value[q] = (1.0 - go) * leaf_q + go * value[q]
        value[1 - q] = leaf_o + value[1 - q]
        for p in range(2):
            at = (2 * s + p) * ROWS
            nsc[at : at + ROWS, :] = jnp.where(inside, value[p], 1.0) * alive_rows
            half = (2 * s + p) * HALF
            rsend[half : half + TILES, :] = nsc[at : at + TILES, :] + nsc[at + TILES : at + 2 * TILES, :]

    def r_copy(dc, db):
        to_core = (core + dc) % 2
        to_col = (col + db) % COLUMNS
        to = 2 * node + to_core
        s = (to_col + to) % SECTIONS
        return remote(
            slot(rsend, 2 * s + to_core, HALF), slot(rrecv, dc * COLUMNS + db, HALF), r_ss.at[dc * COLUMNS + db],
            r_rs.at[dc * COLUMNS + db], to, to_col,
        )

    pairs = [(dc, db) for db in range(COLUMNS) for dc in range(2) if dc or db]
    for dc, db in pairs:
        r_copy(dc, db).start()

    def g_copy(to):
        return remote(
            slot(gsend, to, ROWS), slot(grecv, me, ROWS), g_ss.at[to], g_rs.at[me], to, col
        )

    for d in order:
        g_copy((me + d) % SECTIONS).start()
    grecv[own, :] = gsend[own, :]

    mine = (col + me) % SECTIONS
    total = rsend[pl.ds(pl.multiple_of((2 * mine + core) * HALF, 8), HALF), :]
    for dc, db in pairs:
        r_copy(dc, db).wait_recv()
        at = (dc * COLUMNS + db) * HALF
        total = total + rrecv[at : at + HALF, :]
    fsend[...] = total / total[TILES - 1 : TILES, 127:128]

    def f_copy(db):
        return remote(slot(fsend, 0, HALF), slot(frecv, me, HALF), f_ss.at[db], f_rs.at[me], mine, (col + db) % COLUMNS)

    for db in range(1, COLUMNS):
        f_copy(db).start()

    @pl.when(col != 0)
    def _():
        f_copy(0).start()

    @pl.when(col == 0)
    def _():
        frecv[pl.ds(pl.multiple_of(me * HALF, 8), HALF), :] = fsend[...]

    for d in range(1, SECTIONS):
        other = (me + d) % SECTIONS
        remote(slot(gsend, other, ROWS), slot(grecv, other, ROWS), g_ss.at[other], g_rs.at[other], other, col).wait_recv()
    for j in range(BOARD_DEV):
        keep = live_s[j] > 0
        for t in range(TILES):
            size = 128 if t < TILES - 1 else LAST
            at = pl.ds(128 * t, size)
            gap = grecv[pl.ds((j // 2) * ROWS + (j % 2) * TILES + t, NODES, stride=2 * ROWS), :][:, :size]
            stop = stop_v[j, :, at]
            go = go_v[j, :, at]
            total_regret = stop + go
            out_stop[j, :, at] = jnp.where(keep, jnp.maximum(stop + go / total_regret * gap, 0.0), stop)
            out_go[j, :, at] = jnp.where(keep, jnp.maximum(go - stop / total_regret * gap, 0.0), go)

    for k in range(SECTIONS):
        @pl.when(jnp.logical_or(me != k, col != 0))
        def _(k=k):
            remote(slot(fsend, 0, HALF), slot(frecv, k, HALF), f_ss.at[0], f_rs.at[k], mine, col).wait_recv()
    for p in range(2):
        for t in range(TILES):
            size = 128 if t < TILES - 1 else LAST
            tile = frecv[pl.ds(p * HALF + t, NODES, stride=2 * HALF), :]
            out_sec[p, :, pl.ds(128 * t, size)] = tile[:, :size]

    for d in order:
        a_copy((me + d) % SECTIONS).wait_send()
        g_copy((me + d) % SECTIONS).wait_send()
    for dc, db in pairs:
        r_copy(dc, db).wait_send()
    for db in range(1, COLUMNS):
        f_copy(db).wait_send()

    @pl.when(col != 0)
    def _():
        f_copy(0).wait_send()


def local(root_reach, frontier_value, regret_stop, regret_go, board_live, board_cards, hand_rank):
    bits, scan = hand_bits()
    f32, i32 = jnp.float32, jnp.int32
    regrets = (BOARD_DEV, NODES, H)
    ends = (2, NODES, H)
    any_spec = pl.BlockSpec(memory_space=pl.ANY)
    vmem_spec = pl.BlockSpec(memory_space=pltpu.VMEM)
    dma = pltpu.SemaphoreType.DMA
    new_stop, new_go, section_value = pl.pallas_call(
        kernel,
        out_shape=(
            jax.ShapeDtypeStruct(regrets, f32),
            jax.ShapeDtypeStruct(regrets, f32),
            jax.ShapeDtypeStruct(ends, f32),
        ),
        in_specs=[any_spec] * 9,
        out_specs=(vmem_spec,) * 3,
        scratch_shapes=[
            pltpu.VMEM(ends, f32), pltpu.VMEM(ends, f32), pltpu.VMEM(regrets, f32), pltpu.VMEM(regrets, f32),
            pltpu.SMEM((BOARD_DEV,), i32), pltpu.SMEM((BOARD_DEV, 5), i32), pltpu.VMEM((BOARD_DEV, H), i32),
            pltpu.VMEM((2, HP), i32), pltpu.VMEM((2 * ROWS, 128), i32),
            pltpu.VMEM((BOARD_DEV, NODES, 128), f32),
            pltpu.VMEM((SECTIONS * ROWS, 128), f32), pltpu.VMEM((SECTIONS * ROWS, 128), f32),
            pltpu.VMEM((4 * NODES * ROWS, 128), f32),
            pltpu.VMEM((8, HP), i32), pltpu.VMEM((8, HP), f32), pltpu.VMEM((2, 8, HP), i32), pltpu.VMEM((2, 8, HP), f32),
            pltpu.VMEM((HP, 8), i32), pltpu.VMEM((HP, 8), f32),
            pltpu.VMEM((2, HP, HP), jnp.bfloat16),
            pltpu.VMEM((2, SECTIONS * ROWS, 128), f32), pltpu.VMEM((2, 2 * SECTIONS, HP), jnp.bfloat16),
            pltpu.VMEM((2, SECTIONS * ROWS, 128), f32),
            pltpu.VMEM((SECTIONS * ROWS, 128), f32), pltpu.VMEM((SECTIONS * ROWS, 128), f32),
            pltpu.VMEM((2 * SECTIONS * ROWS, 128), f32),
            pltpu.VMEM((2 * SECTIONS * HALF, 128), f32), pltpu.VMEM((2 * COLUMNS * HALF, 128), f32),
            pltpu.VMEM((HALF, 128), f32), pltpu.VMEM((SECTIONS * HALF, 128), f32),
            dma((9,)), dma((SECTIONS,)), dma((SECTIONS,)), dma((SECTIONS,)), dma((SECTIONS,)),
            dma((2 * COLUMNS,)), dma((2 * COLUMNS,)), dma((COLUMNS,)), dma((SECTIONS,)),
        ],
        compiler_params=pltpu.CompilerParams(
            collective_id=0, has_side_effects=True, vmem_limit_bytes=67043328
        ),
    )(
        root_reach, frontier_value, regret_stop[0], regret_go[0], board_live, board_cards, hand_rank,
        jnp.asarray(bits), jnp.asarray(scan),
    )
    return new_stop[None], new_go[None], section_value[None]


def solution(mesh):
    regrets = P("section", "board", None, None)
    return jax.shard_map(
        local,
        mesh=mesh,
        in_specs=(P(), P(), regrets, regrets, P("board"), P("board", None), P("board", None)),
        out_specs=(regrets, regrets, P("section", None, None, None)),
        check_vma=False,
    )
```

```python
import jax
import jax.numpy as jnp
import numpy as np
from jax import lax
from jax.experimental import pallas as pl
from jax.experimental.pallas import tpu as pltpu
from jax.sharding import PartitionSpec as P

CARDS = 52
H = 1326
NODES = 8
TILES = 11
HP = TILES * 128
LAST = H - 128 * (TILES - 1)
SECTIONS = 16
COLUMNS = 16
BOARD_DEV = 4
ROWS = 24
BLOCK = 64
HALF = 16
MESH = pl.DeviceIdType.MESH
FAR = sorted(range(COLUMNS), key=lambda d: -min(d // 4, 4 - d // 4) - min(d % 4, 4 - d % 4))


def hand_bits():
    first, second = np.triu_indices(CARDS, 1)
    low = np.full((HP,), -1, np.int64)
    high = np.full((HP,), -1, np.int64)
    both = (np.int64(1) << first) | (np.int64(1) << second)
    low[:H] = both & 0xFFFFFFFF
    high[:H] = both >> 32
    rows = np.stack([low, high]).astype(np.uint32).view(np.int32)
    scan = np.full((2, ROWS, 128), -1, np.int32)
    for word in range(2):
        tiles = rows[word].reshape(TILES, 128)
        scan[word, :TILES] = tiles
        scan[word, TILES : 2 * TILES] = tiles
    return rows, scan.reshape(2 * ROWS, 128)


def remote(src, dst, send, recv, section, board):
    return pltpu.make_async_remote_copy(
        src_ref=src,
        dst_ref=dst,
        send_sem=send,
        recv_sem=recv,
        device_id={"section": section, "board": board},
        device_id_type=MESH,
    )


def slot(ref, index, rows):
    used = 2 * TILES if rows == ROWS else TILES
    return ref.at[pl.ds(pl.multiple_of(index * rows, 8), used), :]


def wait_rows(ref, rows, sem):
    some = ref.at[pl.ds(0, rows), :]
    pltpu.make_async_copy(some, some, sem).wait()


def kernel(
    root_hbm, front_hbm, stop_hbm, go_hbm, live_hbm, cards_hbm, rank_hbm, bits_hbm, scan_hbm,
    out_stop, out_go, out_sec,
    root_v, front_v, regret_v, live_s, cards_s, rank_v, bits_v, scan_v,
    pad, asend, arecv, ends, bitrow, rankrow, bitwide, rankwide, bitcol, rankcol, w, lsc, lhs, leafsc,
    gsend, grecv, nsc, rsend, rrecv, fsend, frecv,
    in_sem, regret_sem, a_ss, a_rs, g_ss, g_rs, r_ss, r_rs, f_ss, f_rs,
):
    me = lax.axis_index("section")
    col = lax.axis_index("board")
    node = me // 2
    core = me % 2
    row, lane = col // 4, col % 4

    def column(db):
        return (row + db // 4) % 4 * 4 + (lane + db % 4) % 4

    loads = [
        pltpu.make_async_copy(src, dst, in_sem.at[i])
        for i, (src, dst) in enumerate(
            [
                (root_hbm, root_v), (front_hbm, front_v),
                (live_hbm, live_s), (cards_hbm, cards_s), (rank_hbm, rank_v), (bits_hbm, bits_v),
                (scan_hbm, scan_v),
            ]
        )
    ]
    for i, src in enumerate((stop_hbm, go_hbm)):
        pltpu.make_async_copy(src, regret_v.at[i], regret_sem).start()
    for copy in loads:
        copy.start()
    barrier = pltpu.get_barrier_semaphore()
    for d in range(1, SECTIONS):
        pl.semaphore_signal(
            barrier, inc=1, device_id={"section": (me + d) % SECTIONS, "board": col}, device_id_type=MESH
        )
    for dc in range(2):
        for db in range(1, COLUMNS):
            pl.semaphore_signal(
                barrier,
                inc=1,
                device_id={"section": 2 * node + (core + dc) % 2, "board": column(db)},
                device_id_type=MESH,
            )

    pad[...] = jnp.full(pad.shape, 0.5, jnp.float32)
    ends[...] = jnp.zeros(ends.shape, jnp.float32)
    pltpu.make_async_copy(regret_v, regret_v, regret_sem).wait()

    for j in range(BOARD_DEV):
        for t in range(TILES):
            if t < TILES - 1:
                at = pl.ds(128 * t, 128)
                tile = regret_v[1, j, :, at] / (regret_v[1, j, :, at] + regret_v[0, j, :, at])
            else:
                at = pl.ds(128 * t, LAST)
                pad[j, :, :LAST] = regret_v[1, j, :, at] / (regret_v[1, j, :, at] + regret_v[0, j, :, at])
                tile = pad[j]
            at_row = (j // 2) * ROWS + (j % 2) * TILES + t
            asend[pl.ds(at_row, NODES, stride=2 * ROWS), :] = tile
    pl.semaphore_wait(barrier, SECTIONS - 1 + 2 * (COLUMNS - 1))

    def a_copy(to):
        return remote(
            slot(asend, to, ROWS), slot(arecv, me, ROWS), a_ss, a_rs, to, col
        )

    order = sorted(range(1, SECTIONS), key=lambda d: -min(d, SECTIONS - d))
    for d in order:
        a_copy((me + d) % SECTIONS).start()
    own = pl.ds(pl.multiple_of(me * ROWS, 8), ROWS)
    arecv[own, :] = asend[own, :]

    for copy in loads:
        copy.wait()

    alive = []
    board_bits = []
    for jj in range(2):
        j = 2 * core + jj
        alive.append(jnp.where(live_s[j] > 0, 1.0, 0.0).astype(jnp.float32))
        low = jnp.int32(0)
        high = jnp.int32(0)
        for i in range(5):
            card = cards_s[j, i]
            bit = lax.shift_left(jnp.int32(1), card % 32)
            low = low | jnp.where(card < 32, bit, 0)
            high = high | jnp.where(card < 32, 0, bit)
        board_bits.append((low, high))
    row_id = lax.broadcasted_iota(jnp.int32, (ROWS, 128), 0)
    first_slot = row_id < TILES
    low = jnp.where(first_slot, board_bits[0][0], board_bits[1][0])
    high = jnp.where(first_slot, board_bits[0][1], board_bits[1][1])
    hit = (scan_v[:ROWS, :] & low) | (scan_v[ROWS:, :] & high)
    mask = jnp.where(hit == 0, 1.0, 0.0).astype(jnp.float32)
    inside = (scan_v[:ROWS, :] & scan_v[ROWS:, :]) != -1
    alive_rows = jnp.where(first_slot, alive[0], alive[1])

    for which, ref in enumerate((root_v, front_v)):
        for p in range(2):
            base = (2 * which + p) * NODES * ROWS
            pad[p, :, :] = jnp.zeros((NODES, 128), jnp.float32)
            pad[p, :, :LAST] = ref[p, :, pl.ds(128 * (TILES - 1), LAST)]
            for t in range(TILES):
                tile = ref[p, :, pl.ds(128 * t, 128)] if t < TILES - 1 else pad[p]
                ends[pl.ds(base + t, NODES, stride=ROWS), :] = tile
                ends[pl.ds(base + TILES + t, NODES, stride=ROWS), :] = tile

    def end_of(index):
        at = pl.multiple_of((index * NODES + node) * ROWS, 8)
        return jnp.where(mask > 0, ends[pl.ds(at, ROWS), :], 0.0)

    bitrow[...] = jnp.zeros(bitrow.shape, jnp.int32)
    bitrow[0:2, :] = bits_v[...]
    rankrow[...] = jnp.zeros(rankrow.shape, jnp.float32)
    for jj in range(2):
        rankrow[jj : jj + 1, :H] = rank_v[pl.ds(2 * core + jj, 1), :].astype(jnp.float32)
    for r in range(2):
        bitwide[r] = jnp.broadcast_to(bitrow[r : r + 1, :], (8, HP))
        rankwide[r] = jnp.broadcast_to(rankrow[r : r + 1, :], (8, HP))
    for t in range(TILES):
        lanes = slice(128 * t, 128 * (t + 1))
        bitcol[lanes, :] = bitrow[:, lanes].T
        rankcol[lanes, :] = rankrow[:, lanes].T

    def payoff_rows(block, _):
        at = [pl.multiple_of(block * BLOCK + 16 * i, 16) for i in range(BLOCK // 16)]
        wide = [
            [jnp.broadcast_to(ref[pl.ds(a, 16), r : r + 1], (16, 128)) for ref in (bitcol, rankcol) for r in range(2)]
            for a in at
        ]
        one = jnp.bfloat16(1)
        for t in range(TILES):
            lanes = slice(128 * t, 128 * (t + 1))
            low, high, rank0, rank1 = (
                jnp.concatenate([ref[r, :, lanes]] * 2, axis=0) for ref in (bitwide, rankwide) for r in range(2)
            )
            for a, (low_g, high_g, rank0_g, rank1_g) in zip(at, wide):
                shared = (low_g & low) | (high_g & high)
                free = jnp.where(shared == 0, 1.0, 0.0).astype(jnp.bfloat16)
                for jj, step in enumerate((rank0 - rank0_g, rank1 - rank1_g)):
                    step = step.astype(jnp.bfloat16)
                    w[jj, pl.ds(a, 16), lanes] = jnp.minimum(jnp.maximum(step, -one), one) * free
        return 0

    lax.fori_loop(0, HP // BLOCK, payoff_rows, 0)

    wait_rows(arecv, (SECTIONS - 1) * 2 * TILES, a_rs)

    reach = [end_of(0), end_of(1)]
    for s in range(SECTIONS):
        go = jnp.where(inside, arecv[s * ROWS : (s + 1) * ROWS, :], 0.5)
        q = s % 2
        lsc[q, s * ROWS : (s + 1) * ROWS, :] = reach[q] * (1.0 - go)
        lsc[1 - q, s * ROWS : (s + 1) * ROWS, :] = reach[1 - q]
        reach[q] = reach[q] * go
    for jj in range(2):
        for p in range(2):
            for t in range(TILES):
                tile = lsc[p, pl.ds(jj * TILES + t, SECTIONS, stride=ROWS), :]
                lhs[jj, p * SECTIONS : (p + 1) * SECTIONS, 128 * t : 128 * (t + 1)] = tile.astype(jnp.bfloat16)
    for jj in range(2):
        leaf = jnp.dot(lhs[jj], w[jj], preferred_element_type=jnp.float32)
        for p in range(2):
            for t in range(TILES):
                tile = leaf[p * SECTIONS : (p + 1) * SECTIONS, 128 * t : 128 * (t + 1)]
                leafsc[1 - p, pl.ds(jj * TILES + t, SECTIONS, stride=ROWS), :] = tile

    value = [end_of(2), end_of(3)]
    for s in reversed(range(SECTIONS)):
        q = s % 2
        rows = slice(s * ROWS, (s + 1) * ROWS)
        go = jnp.where(inside, arecv[rows, :], 0.5)
        leaf_q = leafsc[q, rows, :] * mask
        leaf_o = leafsc[1 - q, rows, :] * mask
        gsend[rows, :] = leaf_q - value[q]
        value[q] = (1.0 - go) * leaf_q + go * value[q]
        value[1 - q] = leaf_o + value[1 - q]
        for p in range(2):
            at = (2 * s + p) * ROWS
            nsc[at : at + ROWS, :] = jnp.where(inside, value[p], 1.0) * alive_rows
            half = (2 * s + p) * HALF
            rsend[half : half + TILES, :] = nsc[at : at + TILES, :] + nsc[at + TILES : at + 2 * TILES, :]

    def r_copy(dc, db):
        to_core = (core + dc) % 2
        to_col = column(db)
        to = 2 * node + to_core
        s = (to_col + to) % SECTIONS
        return remote(
            slot(rsend, 2 * s + to_core, HALF), slot(rrecv, dc * COLUMNS + db, HALF), r_ss, r_rs, to, to_col,
        )

    pairs = [(dc, db) for db in FAR for dc in range(2) if dc or db]
    for dc, db in pairs:
        r_copy(dc, db).start()

    def g_copy(to):
        return remote(
            slot(gsend, to, ROWS), slot(grecv, me, ROWS), g_ss, g_rs, to, col
        )

    for d in order:
        g_copy((me + d) % SECTIONS).start()
    grecv[own, :] = gsend[own, :]

    mine = (col + me) % SECTIONS
    total = rsend[pl.ds(pl.multiple_of((2 * mine + core) * HALF, 8), HALF), :]
    wait_rows(rrecv, (2 * COLUMNS - 1) * TILES, r_rs)
    for dc, db in pairs:
        at = (dc * COLUMNS + db) * HALF
        total = total + rrecv[at : at + HALF, :]
    fsend[...] = total / total[TILES - 1 : TILES, 127:128]

    def f_copy(db):
        return remote(slot(fsend, 0, HALF), slot(frecv, me, HALF), f_ss, f_rs, mine, column(db))

    for db in FAR[:-1]:
        f_copy(db).start()

    @pl.when(col != 0)
    def _():
        f_copy(0).start()

    @pl.when(col == 0)
    def _():
        frecv[pl.ds(pl.multiple_of(me * HALF, 8), HALF), :] = fsend[...]

    wait_rows(grecv, (SECTIONS - 1) * 2 * TILES, g_rs)
    for j in range(BOARD_DEV):
        keep = live_s[j] > 0
        for t in range(TILES):
            size = 128 if t < TILES - 1 else LAST
            at = pl.ds(128 * t, size)
            gap = grecv[pl.ds((j // 2) * ROWS + (j % 2) * TILES + t, NODES, stride=2 * ROWS), :][:, :size]
            stop = regret_v[0, j, :, at]
            go = regret_v[1, j, :, at]
            total_regret = stop + go
            out_stop[j, :, at] = jnp.where(keep, jnp.maximum(stop + go / total_regret * gap, 0.0), stop)
            out_go[j, :, at] = jnp.where(keep, jnp.maximum(go - stop / total_regret * gap, 0.0), go)

    wait_rows(asend, (SECTIONS - 1) * 2 * TILES, a_ss)
    wait_rows(gsend, (SECTIONS - 1) * 2 * TILES, g_ss)
    wait_rows(rsend, (2 * COLUMNS - 1) * TILES, r_ss)

    @pl.when(col != 0)
    def _():
        wait_rows(frecv, COLUMNS * TILES, f_ss)

    @pl.when(col == 0)
    def _():
        wait_rows(frecv, (COLUMNS - 1) * TILES, f_ss)

    @pl.when(col != 0)
    def _():
        wait_rows(frecv, SECTIONS * TILES, f_rs)

    @pl.when(col == 0)
    def _():
        wait_rows(frecv, (SECTIONS - 1) * TILES, f_rs)

    for p in range(2):
        for t in range(TILES):
            size = 128 if t < TILES - 1 else LAST
            tile = frecv[pl.ds(p * HALF + t, NODES, stride=2 * HALF), :]
            out_sec[p, :, pl.ds(128 * t, size)] = tile[:, :size]


def store(stop_v, go_v, sec_v, out_stop, out_go, out_sec, sem):
    pairs = ((stop_v, out_stop), (go_v, out_go), (sec_v, out_sec))
    copies = [pltpu.make_async_copy(src, dst.at[0], sem.at[i]) for i, (src, dst) in enumerate(pairs)]
    for copy in copies:
        copy.start()
    for copy in copies:
        copy.wait()


def local(root_reach, frontier_value, regret_stop, regret_go, board_live, board_cards, hand_rank):
    bits, scan = hand_bits()
    f32, i32 = jnp.float32, jnp.int32
    regrets = (BOARD_DEV, NODES, H)
    ends = (2, NODES, H)
    hbm_spec = pl.BlockSpec(memory_space=pltpu.HBM)
    vmem_spec = pl.BlockSpec(memory_space=pltpu.VMEM)
    dma = pltpu.SemaphoreType.DMA
    operands = (
        root_reach, frontier_value, regret_stop[0], regret_go[0], board_live, board_cards, hand_rank,
        jnp.asarray(bits), jnp.asarray(scan),
    )
    new_stop, new_go, section_value = pl.pallas_call(
        kernel,
        out_shape=(
            pltpu.VMEM(regrets, f32),
            pltpu.VMEM(regrets, f32),
            pltpu.VMEM(ends, f32),
        ),
        in_specs=[hbm_spec] * 9,
        out_specs=(vmem_spec,) * 3,
        scratch_shapes=[
            pltpu.VMEM(ends, f32), pltpu.VMEM(ends, f32), pltpu.VMEM((2, *regrets), f32),
            pltpu.SMEM((BOARD_DEV,), i32), pltpu.SMEM((BOARD_DEV, 5), i32), pltpu.VMEM((BOARD_DEV, H), i32),
            pltpu.VMEM((2, HP), i32), pltpu.VMEM((2 * ROWS, 128), i32),
            pltpu.VMEM((BOARD_DEV, NODES, 128), f32),
            pltpu.VMEM((SECTIONS * ROWS, 128), f32), pltpu.VMEM((SECTIONS * ROWS, 128), f32),
            pltpu.VMEM((4 * NODES * ROWS, 128), f32),
            pltpu.VMEM((8, HP), i32), pltpu.VMEM((8, HP), f32), pltpu.VMEM((2, 8, HP), i32), pltpu.VMEM((2, 8, HP), f32),
            pltpu.VMEM((HP, 8), i32), pltpu.VMEM((HP, 8), f32),
            pltpu.VMEM((2, HP, HP), jnp.bfloat16),
            pltpu.VMEM((2, SECTIONS * ROWS, 128), f32), pltpu.VMEM((2, 2 * SECTIONS, HP), jnp.bfloat16),
            pltpu.VMEM((2, SECTIONS * ROWS, 128), f32),
            pltpu.VMEM((SECTIONS * ROWS, 128), f32), pltpu.VMEM((SECTIONS * ROWS, 128), f32),
            pltpu.VMEM((2 * SECTIONS * ROWS, 128), f32),
            pltpu.VMEM((2 * SECTIONS * HALF, 128), f32), pltpu.VMEM((2 * COLUMNS * HALF, 128), f32),
            pltpu.VMEM((HALF, 128), f32), pltpu.VMEM((SECTIONS * HALF, 128), f32),
            dma((7,)), *([dma] * 9),
        ],
        compiler_params=pltpu.CompilerParams(
            collective_id=0, has_side_effects=True, vmem_limit_bytes=32 * 1024 * 1024
        ),
    )(*(pltpu.with_memory_space_constraint(x, pltpu.HBM) for x in operands))
    return pl.pallas_call(
        store,
        out_shape=(
            jax.ShapeDtypeStruct((1, *regrets), f32),
            jax.ShapeDtypeStruct((1, *regrets), f32),
            jax.ShapeDtypeStruct((1, *ends), f32),
        ),
        in_specs=[vmem_spec] * 3,
        out_specs=(hbm_spec,) * 3,
        scratch_shapes=[dma((3,))],
        compiler_params=pltpu.CompilerParams(vmem_limit_bytes=1024 * 1024),
    )(new_stop, new_go, section_value)


def solution(mesh):
    regrets = P("section", "board", None, None)
    return jax.shard_map(
        local,
        mesh=mesh,
        in_specs=(P(), P(), regrets, regrets, P("board"), P("board", None), P("board", None)),
        out_specs=(regrets, regrets, P("section", None, None, None)),
        check_vma=False,
    )
```

```python
import jax
import jax.numpy as jnp
import numpy as np
from jax import lax
from jax.experimental import pallas as pl
from jax.experimental.pallas import tpu as pltpu
from jax.sharding import PartitionSpec as P

CARDS = 52
H = 1326
NODES = 8
TILES = 11
HP = TILES * 128
LAST = H - 128 * (TILES - 1)
SECTIONS = 16
COLUMNS = 16
BOARD_DEV = 4
UNIT = 24
BLOCK = 32
HALF = 16
MESH = pl.DeviceIdType.MESH
ORDER = sorted(range(1, SECTIONS), key=lambda d: -min(d, SECTIONS - d))
FAR = sorted(range(COLUMNS), key=lambda d: -min(d // 4, 4 - d // 4) - min(d % 4, 4 - d % 4))


def hand_bits():
    first, second = np.triu_indices(CARDS, 1)
    low = np.full((HP,), -1, np.int64)
    high = np.full((HP,), -1, np.int64)
    both = (np.int64(1) << first) | (np.int64(1) << second)
    low[:H] = both & 0xFFFFFFFF
    high[:H] = both >> 32
    rows = np.stack([low, high]).astype(np.uint32).view(np.int32)
    return rows, rows.reshape(2, TILES, 128)


def remote(src, dst, send, recv, section, board):
    return pltpu.make_async_remote_copy(
        src_ref=src,
        dst_ref=dst,
        send_sem=send,
        recv_sem=recv,
        device_id={"section": section, "board": board},
        device_id_type=MESH,
    )


def unit(ref, index, stride=UNIT):
    return ref.at[pl.ds(pl.multiple_of(index * stride, 8), TILES), :]


def wait_rows(ref, rows, sem):
    some = ref.at[pl.ds(0, rows), :]
    pltpu.make_async_copy(some, some, sem).wait()


def kernel(
    root_hbm, front_hbm, stop_hbm, go_hbm, live_hbm, cards_hbm, rank_hbm, bits_hbm, scan_hbm,
    out_stop, out_go, out_sec,
    root_v, front_v, regret_v, live_s, cards_s, rank_v, bits_v, scan_v,
    pad, asend, arecv, ends, bitrow, rankrow, bitwide, rankwide, bitcol, rankcol, w, lsc, lhs, leafsc,
    gsend, grecv, rsend, rrecv, fsend, frecv,
    in_sem, regret_sem, a_ss, a_rs, g_ss, g_rs, r_ss, r_rs, f_ss, f_rs,
):
    me = lax.axis_index("section")
    col = lax.axis_index("board")
    node = me // 2
    core = me % 2
    row, lane = col // 4, col % 4

    def column(db):
        return (row + db // 4) % 4 * 4 + (lane + db % 4) % 4

    loads = [
        pltpu.make_async_copy(src, dst, in_sem.at[i])
        for i, (src, dst) in enumerate(
            [
                (root_hbm, root_v), (front_hbm, front_v),
                (live_hbm, live_s), (cards_hbm, cards_s), (rank_hbm, rank_v), (bits_hbm, bits_v),
                (scan_hbm, scan_v),
            ]
        )
    ]
    for i, src in enumerate((stop_hbm, go_hbm)):
        pltpu.make_async_copy(src, regret_v.at[i], regret_sem).start()
    for copy in loads:
        copy.start()
    barrier = pltpu.get_barrier_semaphore()

    def greet(section, board):
        pl.semaphore_signal(barrier, inc=1, device_id={"section": section, "board": board}, device_id_type=MESH)

    for d in ORDER:
        greet((me + d) % SECTIONS, col)
    for db in FAR[:-1]:
        for dc in range(2):
            greet(2 * node + (core + dc) % 2, column(db))
    pad[...] = jnp.full(pad.shape, 0.5, jnp.float32)
    ends[...] = jnp.zeros(ends.shape, jnp.float32)
    pltpu.make_async_copy(regret_v, regret_v, regret_sem).wait()

    for j in range(BOARD_DEV):
        for t in range(TILES):
            if t < TILES - 1:
                at = pl.ds(128 * t, 128)
                tile = regret_v[1, j, :, at] / (regret_v[1, j, :, at] + regret_v[0, j, :, at])
            else:
                at = pl.ds(128 * t, LAST)
                pad[j, :, :LAST] = regret_v[1, j, :, at] / (regret_v[1, j, :, at] + regret_v[0, j, :, at])
                tile = pad[j]
            first = (j % 2 * 2 + j // 2) * NODES * UNIT
            asend[pl.ds(first + t, NODES, stride=UNIT), :] = tile
    for copy in loads:
        copy.wait()

    alive = []
    board_bits = []
    for jj in range(2):
        j = 2 * core + jj
        alive.append(jnp.where(live_s[j] > 0, 1.0, 0.0).astype(jnp.float32))
        low = jnp.int32(0)
        high = jnp.int32(0)
        for i in range(5):
            card = cards_s[j, i]
            bit = lax.shift_left(jnp.int32(1), card % 32)
            low = low | jnp.where(card < 32, bit, 0)
            high = high | jnp.where(card < 32, 0, bit)
        board_bits.append((low, high))
    inside = (scan_v[0] & scan_v[1]) != -1
    mask = [
        jnp.where(((scan_v[0] & low) | (scan_v[1] & high)) == 0, 1.0, 0.0).astype(jnp.float32)
        for low, high in board_bits
    ]

    for which, ref in enumerate((root_v, front_v)):
        for p in range(2):
            base = (2 * which + p) * NODES * UNIT
            pad[p, :, :] = jnp.zeros((NODES, 128), jnp.float32)
            pad[p, :, :LAST] = ref[p, :, pl.ds(128 * (TILES - 1), LAST)]
            for t in range(TILES):
                tile = ref[p, :, pl.ds(128 * t, 128)] if t < TILES - 1 else pad[p]
                ends[pl.ds(base + t, NODES, stride=UNIT), :] = tile

    def end_of(index, jj):
        return unit(ends, index * NODES + node)[...] * mask[jj]

    bitrow[...] = jnp.zeros(bitrow.shape, jnp.int32)
    bitrow[0:2, :] = bits_v[...]
    rankrow[...] = jnp.zeros(rankrow.shape, jnp.float32)
    for jj in range(2):
        rankrow[jj : jj + 1, :H] = rank_v[pl.ds(2 * core + jj, 1), :].astype(jnp.float32)
    for r in range(2):
        bitwide[r] = jnp.broadcast_to(bitrow[r : r + 1, :], (8, HP))
        rankwide[r] = jnp.broadcast_to(rankrow[r : r + 1, :], (8, HP))
    for t in range(TILES):
        lanes = slice(128 * t, 128 * (t + 1))
        bitcol[lanes, :] = bitrow[:, lanes].T
        rankcol[lanes, :] = rankrow[:, lanes].T

    pl.semaphore_wait(barrier, SECTIONS - 1 + 2 * (COLUMNS - 1))

    def a_unit(jj, to):
        return (2 * jj + to % 2) * NODES + to // 2

    def a_copy(jj, to):
        return remote(
            unit(asend, a_unit(jj, to)), unit(arecv, jj * SECTIONS + me), a_ss, a_rs.at[jj], to, col
        )

    for jj in range(2):
        for d in ORDER:
            a_copy(jj, (me + d) % SECTIONS).start()
    for jj in range(2):
        unit(arecv, jj * SECTIONS + me)[...] = unit(asend, a_unit(jj, me))[...]

    def payoff_rows(block, _):
        at = [pl.multiple_of(block * BLOCK + 16 * i, 16) for i in range(BLOCK // 16)]
        wide = [
            [jnp.broadcast_to(ref[pl.ds(a, 16), r : r + 1], (16, 128)) for ref in (bitcol, rankcol) for r in range(2)]
            for a in at
        ]
        one = jnp.bfloat16(1)
        for t in range(TILES):
            lanes = slice(128 * t, 128 * (t + 1))
            low, high, rank0, rank1 = (
                jnp.concatenate([ref[r, :, lanes]] * 2, axis=0) for ref in (bitwide, rankwide) for r in range(2)
            )
            for a, (low_g, high_g, rank0_g, rank1_g) in zip(at, wide):
                shared = (low_g & low) | (high_g & high)
                free = jnp.where(shared == 0, 1.0, 0.0).astype(jnp.bfloat16)
                for jj, step in enumerate((rank0 - rank0_g, rank1 - rank1_g)):
                    step = step.astype(jnp.bfloat16)
                    w[jj, pl.ds(a, 16), lanes] = jnp.minimum(jnp.maximum(step, -one), one) * free
        return 0

    lax.fori_loop(0, HP // BLOCK, payoff_rows, 0, unroll=2)

    for jj in range(2):
        wait_rows(arecv, (SECTIONS - 1) * TILES, a_rs.at[jj])
        reach = [end_of(0, jj), end_of(1, jj)]
        for s in range(SECTIONS):
            go = jnp.where(inside, unit(arecv, jj * SECTIONS + s)[...], 0.5)
            q = s % 2
            unit(lsc, (2 * jj + q) * SECTIONS + s)[...] = reach[q] * (1.0 - go)
            unit(lsc, (2 * jj + 1 - q) * SECTIONS + s)[...] = reach[1 - q]
            reach[q] = reach[q] * go
        for p in range(2):
            for t in range(TILES):
                tile = lsc[pl.ds((2 * jj + p) * SECTIONS * UNIT + t, SECTIONS, stride=UNIT), :]
                lhs[jj, p * SECTIONS : (p + 1) * SECTIONS, 128 * t : 128 * (t + 1)] = tile.astype(jnp.bfloat16)
        leaf = jnp.dot(lhs[jj], w[jj], preferred_element_type=jnp.float32)
        for p in range(2):
            for t in range(TILES):
                tile = leaf[p * SECTIONS : (p + 1) * SECTIONS, 128 * t : 128 * (t + 1)]
                leafsc[pl.ds((2 * jj + 1 - p) * SECTIONS * UNIT + t, SECTIONS, stride=UNIT), :] = tile

    value = [[end_of(2, jj), end_of(3, jj)] for jj in range(2)]
    for s in reversed(range(SECTIONS)):
        q = s % 2
        for jj in range(2):
            go = jnp.where(inside, unit(arecv, jj * SECTIONS + s)[...], 0.5)
            leaf_q = unit(leafsc, (2 * jj + q) * SECTIONS + s)[...] * mask[jj]
            leaf_o = unit(leafsc, (2 * jj + 1 - q) * SECTIONS + s)[...] * mask[jj]
            unit(gsend, jj * SECTIONS + s)[...] = leaf_q - value[jj][q]
            value[jj][q] = (1.0 - go) * leaf_q + go * value[jj][q]
            value[jj][1 - q] = leaf_o + value[jj][1 - q]
        for p in range(2):
            unit(rsend, 2 * s + p, HALF)[...] = sum(
                jnp.where(inside, value[jj][p], 1.0) * alive[jj] for jj in range(2)
            )

    def r_copy(dc, db):
        to_core = (core + dc) % 2
        to_col = column(db)
        to = 2 * node + to_core
        s = (to_col + 7 * to) % SECTIONS
        return remote(
            unit(rsend, 2 * s + to_core, HALF), unit(rrecv, dc * COLUMNS + db, HALF), r_ss, r_rs, to, to_col,
        )

    pairs = [(dc, db) for db in FAR for dc in range(2) if dc or db]
    for dc, db in pairs:
        r_copy(dc, db).start()

    def g_copy(jj, to):
        return remote(
            unit(gsend, jj * SECTIONS + to), unit(grecv, a_unit(jj, me)), g_ss, g_rs, to, col
        )

    for jj in range(2):
        for d in ORDER:
            g_copy(jj, (me + d) % SECTIONS).start()
    for jj in range(2):
        unit(grecv, a_unit(jj, me))[...] = unit(gsend, jj * SECTIONS + me)[...]

    mine = (col + 7 * me) % SECTIONS
    total = unit(rsend, 2 * mine + core, HALF)[...]
    wait_rows(rrecv, (2 * COLUMNS - 1) * TILES, r_rs)
    for dc, db in pairs:
        total = total + unit(rrecv, dc * COLUMNS + db, HALF)[...]
    fsend[:TILES, :] = total / total[TILES - 1 : TILES, 127:128]

    def f_copy(db):
        return remote(unit(fsend, 0), unit(frecv, me), f_ss, f_rs, mine, column(db))

    for db in FAR[:-1]:
        f_copy(db).start()

    @pl.when(mine != me)
    def _():
        f_copy(0).start()

    @pl.when(mine == me)
    def _():
        unit(frecv, me)[...] = fsend[:TILES, :]

    wait_rows(grecv, (SECTIONS - 1) * 2 * TILES, g_rs)
    for j in range(BOARD_DEV):
        keep = live_s[j] > 0
        for t in range(TILES):
            size = 128 if t < TILES - 1 else LAST
            at = pl.ds(128 * t, size)
            first = (j % 2 * 2 + j // 2) * NODES * UNIT
            gap = grecv[pl.ds(first + t, NODES, stride=UNIT), :][:, :size]
            stop = regret_v[0, j, :, at]
            go = regret_v[1, j, :, at]
            total_regret = stop + go
            out_stop[j, :, at] = jnp.where(keep, jnp.maximum(stop + go / total_regret * gap, 0.0), stop)
            out_go[j, :, at] = jnp.where(keep, jnp.maximum(go - stop / total_regret * gap, 0.0), go)

    wait_rows(asend, (SECTIONS - 1) * 2 * TILES, a_ss)
    wait_rows(gsend, (SECTIONS - 1) * 2 * TILES, g_ss)
    wait_rows(rsend, (2 * COLUMNS - 1) * TILES, r_ss)

    @pl.when(mine != me)
    def _():
        wait_rows(frecv, COLUMNS * TILES, f_ss)

    @pl.when(mine == me)
    def _():
        wait_rows(frecv, (COLUMNS - 1) * TILES, f_ss)

    @pl.when(mine != me)
    def _():
        wait_rows(frecv, SECTIONS * TILES, f_rs)

    @pl.when(mine == me)
    def _():
        wait_rows(frecv, (SECTIONS - 1) * TILES, f_rs)

    for p in range(2):
        for t in range(TILES):
            size = 128 if t < TILES - 1 else LAST
            tile = frecv[pl.ds(p * UNIT + t, NODES, stride=2 * UNIT), :]
            out_sec[p, :, pl.ds(128 * t, size)] = tile[:, :size]


def store(stop_v, go_v, sec_v, out_stop, out_go, out_sec, sem):
    pairs = ((stop_v, out_stop), (go_v, out_go), (sec_v, out_sec))
    copies = [pltpu.make_async_copy(src, dst.at[0], sem.at[i]) for i, (src, dst) in enumerate(pairs)]
    for copy in copies:
        copy.start()
    for copy in copies:
        copy.wait()


def local(root_reach, frontier_value, regret_stop, regret_go, board_live, board_cards, hand_rank):
    bits, scan = hand_bits()
    f32, i32 = jnp.float32, jnp.int32
    regrets = (BOARD_DEV, NODES, H)
    ends = (2, NODES, H)
    hbm_spec = pl.BlockSpec(memory_space=pltpu.HBM)
    vmem_spec = pl.BlockSpec(memory_space=pltpu.VMEM)
    dma = pltpu.SemaphoreType.DMA
    operands = (
        root_reach, frontier_value, regret_stop[0], regret_go[0], board_live, board_cards, hand_rank,
        jnp.asarray(bits), jnp.asarray(scan),
    )
    new_stop, new_go, section_value = pl.pallas_call(
        kernel,
        out_shape=(
            pltpu.VMEM(regrets, f32),
            pltpu.VMEM(regrets, f32),
            pltpu.VMEM(ends, f32),
        ),
        in_specs=[hbm_spec] * 9,
        out_specs=(vmem_spec,) * 3,
        scratch_shapes=[
            pltpu.VMEM(ends, f32), pltpu.VMEM(ends, f32), pltpu.VMEM((2, *regrets), f32),
            pltpu.SMEM((BOARD_DEV,), i32), pltpu.SMEM((BOARD_DEV, 5), i32), pltpu.VMEM((BOARD_DEV, H), i32),
            pltpu.VMEM((2, HP), i32), pltpu.VMEM((2, TILES, 128), i32),
            pltpu.VMEM((BOARD_DEV, NODES, 128), f32),
            pltpu.VMEM((2 * SECTIONS * UNIT, 128), f32), pltpu.VMEM((2 * SECTIONS * UNIT, 128), f32),
            pltpu.VMEM((4 * NODES * UNIT, 128), f32),
            pltpu.VMEM((8, HP), i32), pltpu.VMEM((8, HP), f32), pltpu.VMEM((2, 8, HP), i32), pltpu.VMEM((2, 8, HP), f32),
            pltpu.VMEM((HP, 8), i32), pltpu.VMEM((HP, 8), f32),
            pltpu.VMEM((2, HP, HP), jnp.bfloat16),
            pltpu.VMEM((4 * SECTIONS * UNIT, 128), f32), pltpu.VMEM((2, 2 * SECTIONS, HP), jnp.bfloat16),
            pltpu.VMEM((4 * SECTIONS * UNIT, 128), f32),
            pltpu.VMEM((2 * SECTIONS * UNIT, 128), f32), pltpu.VMEM((2 * SECTIONS * UNIT, 128), f32),
            pltpu.VMEM((2 * SECTIONS * HALF, 128), f32), pltpu.VMEM((2 * COLUMNS * HALF, 128), f32),
            pltpu.VMEM((HALF, 128), f32), pltpu.VMEM((SECTIONS * UNIT, 128), f32),
            dma((7,)), dma, dma, dma((2,)), *([dma] * 6),
        ],
        compiler_params=pltpu.CompilerParams(
            collective_id=0, has_side_effects=True, vmem_limit_bytes=32 * 1024 * 1024
        ),
    )(*(pltpu.with_memory_space_constraint(x, pltpu.HBM) for x in operands))
    return pl.pallas_call(
        store,
        out_shape=(
            jax.ShapeDtypeStruct((1, *regrets), f32),
            jax.ShapeDtypeStruct((1, *regrets), f32),
            jax.ShapeDtypeStruct((1, *ends), f32),
        ),
        in_specs=[vmem_spec] * 3,
        out_specs=(hbm_spec,) * 3,
        scratch_shapes=[dma((3,))],
        compiler_params=pltpu.CompilerParams(vmem_limit_bytes=1024 * 1024),
    )(new_stop, new_go, section_value)


def solution(mesh):
    regrets = P("section", "board", None, None)
    return jax.shard_map(
        local,
        mesh=mesh,
        in_specs=(P(), P(), regrets, regrets, P("board"), P("board", None), P("board", None)),
        out_specs=(regrets, regrets, P("section", None, None, None)),
        check_vma=False,
    )
```

```python
import jax
import jax.numpy as jnp
import numpy as np
from jax import lax
from jax.experimental import pallas as pl
from jax.experimental.pallas import tpu as pltpu
from jax.sharding import PartitionSpec as P

CARDS = 52
H = 1326
NODES = 8
TILES = 11
HP = TILES * 128
LAST = H - 128 * (TILES - 1)
SECTIONS = 16
COLUMNS = 16
BOARD_DEV = 4
UNIT = 24
BLOCK = 64
AHEAD = 2
HALF = 16
MESH = pl.DeviceIdType.MESH
ORDER = sorted(range(1, SECTIONS), key=lambda d: -min(d, SECTIONS - d))
EARLY_SECTIONS = (0, 1, 2, 3, 4, 5, 6, 7, 10, 11, 12, 13, 14, 15, 8, 9)
EARLY_COLUMNS = (0, 1, 3, 4, 2, 8, 5, 12, 7, 9, 6, 13, 11, 15, 10, 14)
FAR = sorted(range(COLUMNS), key=lambda d: -min(d // 4, 4 - d // 4) - min(d % 4, 4 - d % 4))


def hand_bits():
    first, second = np.triu_indices(CARDS, 1)
    low = np.full((HP,), -1, np.int64)
    high = np.full((HP,), -1, np.int64)
    both = (np.int64(1) << first) | (np.int64(1) << second)
    low[:H] = both & 0xFFFFFFFF
    high[:H] = both >> 32
    rows = np.stack([low, high]).astype(np.uint32).view(np.int32)
    return rows, rows.reshape(2, TILES, 128)


def remote(src, dst, send, recv, section, board):
    return pltpu.make_async_remote_copy(
        src_ref=src,
        dst_ref=dst,
        send_sem=send,
        recv_sem=recv,
        device_id={"section": section, "board": board},
        device_id_type=MESH,
    )


def unit(ref, index, stride=UNIT):
    return ref.at[pl.ds(pl.multiple_of(index * stride, 8), TILES), :]


def wait_rows(ref, rows, sem):
    some = ref.at[pl.ds(0, rows), :]
    pltpu.make_async_copy(some, some, sem).wait()


def kernel(
    root_hbm, front_hbm, stop_hbm, go_hbm, live_hbm, cards_hbm, rank_hbm, bits_hbm, scan_hbm,
    out_stop, out_go, out_sec,
    root_v, front_v, regret_v, live_s, cards_s, rank_v, bits_v, scan_v,
    pad, asend, arecv, ends, bitrow, rankrow, bitwide, rankwide, bitcol, rankcol, w, lsc, lhs, leafsc,
    gsend, grecv, rsend, rrecv, fsend, frecv,
    in_sem, regret_sem, a_ss, a_rs, g_ss, g_rs, r_ss, r_rs, f_ss, f_rs,
):
    me = lax.axis_index("section")
    col = lax.axis_index("board")
    node = me // 2
    core = me % 2
    row, lane = col // 4, col % 4

    def column(db):
        return (row + db // 4) % 4 * 4 + (lane + db % 4) % 4

    barrier = pltpu.get_barrier_semaphore()

    def greet(section, board):
        pl.semaphore_signal(barrier, inc=1, device_id={"section": section, "board": board}, device_id_type=MESH)

    for d in ORDER:
        greet((me + d) % SECTIONS, col)
    loads = [
        pltpu.make_async_copy(src, dst, in_sem.at[i])
        for i, (src, dst) in enumerate(
            [
                (root_hbm, root_v), (front_hbm, front_v),
                (live_hbm, live_s), (cards_hbm, cards_s), (rank_hbm, rank_v), (bits_hbm, bits_v),
                (scan_hbm, scan_v),
            ]
        )
    ]
    for i, src in enumerate((stop_hbm, go_hbm)):
        pltpu.make_async_copy(src, regret_v.at[i], regret_sem).start()
    for copy in loads:
        copy.start()
    for db in FAR[:-1]:
        for dc in range(2):
            greet(2 * node + (core + dc) % 2, column(db))
    pad[...] = jnp.full(pad.shape, 0.5, jnp.float32)
    ends[...] = jnp.zeros(ends.shape, jnp.float32)
    pltpu.make_async_copy(regret_v, regret_v, regret_sem).wait()

    for j in range(BOARD_DEV):
        for t in range(TILES):
            if t < TILES - 1:
                at = pl.ds(128 * t, 128)
                tile = regret_v[1, j, :, at] / (regret_v[1, j, :, at] + regret_v[0, j, :, at])
            else:
                at = pl.ds(128 * t, LAST)
                pad[j, :, :LAST] = regret_v[1, j, :, at] / (regret_v[1, j, :, at] + regret_v[0, j, :, at])
                tile = pad[j]
            first = (j % 2 * 2 + j // 2) * NODES * UNIT
            asend[pl.ds(first + t, NODES, stride=UNIT), :] = tile
    for copy in loads:
        copy.wait()

    alive = []
    board_bits = []
    for jj in range(2):
        j = 2 * core + jj
        alive.append(jnp.where(live_s[j] > 0, 1.0, 0.0).astype(jnp.float32))
        low = jnp.int32(0)
        high = jnp.int32(0)
        for i in range(5):
            card = cards_s[j, i]
            bit = lax.shift_left(jnp.int32(1), card % 32)
            low = low | jnp.where(card < 32, bit, 0)
            high = high | jnp.where(card < 32, 0, bit)
        board_bits.append((low, high))
    inside = (scan_v[0] & scan_v[1]) != -1
    mask = [
        jnp.where(((scan_v[0] & low) | (scan_v[1] & high)) == 0, 1.0, 0.0).astype(jnp.float32)
        for low, high in board_bits
    ]

    for which, ref in enumerate((root_v, front_v)):
        for p in range(2):
            base = (2 * which + p) * NODES * UNIT
            pad[p, :, :] = jnp.zeros((NODES, 128), jnp.float32)
            pad[p, :, :LAST] = ref[p, :, pl.ds(128 * (TILES - 1), LAST)]
            for t in range(TILES):
                tile = ref[p, :, pl.ds(128 * t, 128)] if t < TILES - 1 else pad[p]
                ends[pl.ds(base + t, NODES, stride=UNIT), :] = tile

    def end_of(index, jj):
        return unit(ends, index * NODES + node)[...] * mask[jj]

    bitrow[...] = jnp.zeros(bitrow.shape, jnp.int32)
    bitrow[0:2, :] = bits_v[...]
    rankrow[...] = jnp.zeros(rankrow.shape, jnp.float32)
    for jj in range(2):
        rankrow[jj : jj + 1, :H] = rank_v[pl.ds(2 * core + jj, 1), :].astype(jnp.float32)
    for r in range(2):
        bitwide[r] = jnp.broadcast_to(bitrow[r : r + 1, :], (8, HP))
        rankwide[r] = jnp.broadcast_to(rankrow[r : r + 1, :], (8, HP))
    for t in range(TILES):
        lanes = slice(128 * t, 128 * (t + 1))
        bitcol[lanes, :] = bitrow[:, lanes].T
        rankcol[lanes, :] = rankrow[:, lanes].T

    def payoff_rows(block, _):
        at = [pl.multiple_of(block * BLOCK + 16 * i, 16) for i in range(BLOCK // 16)]
        wide = [
            [jnp.broadcast_to(ref[pl.ds(a, 16), r : r + 1], (16, 128)) for ref in (bitcol, rankcol) for r in range(2)]
            for a in at
        ]
        one = jnp.bfloat16(1)
        for t in range(TILES):
            lanes = slice(128 * t, 128 * (t + 1))
            low, high, rank0, rank1 = (
                jnp.concatenate([ref[r, :, lanes]] * 2, axis=0) for ref in (bitwide, rankwide) for r in range(2)
            )
            for a, (low_g, high_g, rank0_g, rank1_g) in zip(at, wide):
                shared = (low_g & low) | (high_g & high)
                free = jnp.where(shared == 0, 1.0, 0.0).astype(jnp.bfloat16)
                for jj, step in enumerate((rank0 - rank0_g, rank1 - rank1_g)):
                    step = step.astype(jnp.bfloat16)
                    w[jj, pl.ds(a, 16), lanes] = jnp.minimum(jnp.maximum(step, -one), one) * free
        return 0

    lax.fori_loop(0, AHEAD, payoff_rows, 0)
    pl.semaphore_wait(barrier, SECTIONS - 1 + 2 * (COLUMNS - 1))

    def a_unit(jj, to):
        return (2 * jj + to % 2) * NODES + to // 2

    def a_copy(jj, to):
        return remote(
            unit(asend, a_unit(jj, to)), unit(arecv, jj * SECTIONS + me), a_ss, a_rs.at[jj], to, col
        )

    for jj in range(2):
        for d in ORDER:
            a_copy(jj, (me + d) % SECTIONS).start()
    for jj in range(2):
        unit(arecv, jj * SECTIONS + me)[...] = unit(asend, a_unit(jj, me))[...]

    lax.fori_loop(AHEAD, HP // BLOCK, payoff_rows, 0)

    for jj in range(2):
        wait_rows(arecv, (SECTIONS - 1) * TILES, a_rs.at[jj])
        reach = [end_of(0, jj), end_of(1, jj)]
        for s in range(SECTIONS):
            go = jnp.where(inside, unit(arecv, jj * SECTIONS + s)[...], 0.5)
            q = s % 2
            unit(lsc, (2 * jj + q) * SECTIONS + s)[...] = reach[q] * (1.0 - go)
            unit(lsc, (2 * jj + 1 - q) * SECTIONS + s)[...] = reach[1 - q]
            reach[q] = reach[q] * go
        for p in range(2):
            for t in range(TILES):
                tile = lsc[pl.ds((2 * jj + p) * SECTIONS * UNIT + t, SECTIONS, stride=UNIT), :]
                lhs[jj, p * SECTIONS : (p + 1) * SECTIONS, 128 * t : 128 * (t + 1)] = tile.astype(jnp.bfloat16)
        leaf = jnp.dot(lhs[jj], w[jj], preferred_element_type=jnp.float32)
        for p in range(2):
            for t in range(TILES):
                tile = leaf[p * SECTIONS : (p + 1) * SECTIONS, 128 * t : 128 * (t + 1)]
                leafsc[pl.ds((2 * jj + 1 - p) * SECTIONS * UNIT + t, SECTIONS, stride=UNIT), :] = tile

    value = [[end_of(2, jj), end_of(3, jj)] for jj in range(2)]
    for s in reversed(range(SECTIONS)):
        q = s % 2
        for jj in range(2):
            go = jnp.where(inside, unit(arecv, jj * SECTIONS + s)[...], 0.5)
            leaf_q = unit(leafsc, (2 * jj + q) * SECTIONS + s)[...] * mask[jj]
            leaf_o = unit(leafsc, (2 * jj + 1 - q) * SECTIONS + s)[...] * mask[jj]
            unit(gsend, jj * SECTIONS + s)[...] = leaf_q - value[jj][q]
            value[jj][q] = (1.0 - go) * leaf_q + go * value[jj][q]
            value[jj][1 - q] = leaf_o + value[jj][1 - q]
        for p in range(2):
            unit(rsend, 2 * s + p, HALF)[...] = sum(
                jnp.where(inside, value[jj][p], 1.0) * alive[jj] for jj in range(2)
            )

    mine = (col + 7 * me) % SECTIONS

    def r_copy(s, p):
        to = 2 * node + p
        return remote(
            unit(rsend, 2 * s + p, HALF), unit(rrecv, core * COLUMNS + col, HALF), r_ss, r_rs,
            to, (s + (SECTIONS - 7) * to) % COLUMNS,
        )

    for s in EARLY_SECTIONS:
        for p in range(2):
            @pl.when(jnp.logical_or(core != p, mine != s))
            def _(s=s, p=p):
                r_copy(s, p).start()

    unit(rrecv, core * COLUMNS + col, HALF)[...] = unit(rsend, 2 * mine + core, HALF)[...]

    def g_copy(jj, to):
        return remote(
            unit(gsend, jj * SECTIONS + to), unit(grecv, a_unit(jj, me)), g_ss, g_rs, to, col
        )

    for jj in range(2):
        for d in ORDER:
            g_copy(jj, (me + d) % SECTIONS).start()
    for jj in range(2):
        unit(grecv, a_unit(jj, me))[...] = unit(gsend, jj * SECTIONS + me)[...]

    wait_rows(rrecv, (2 * COLUMNS - 1) * TILES, r_rs)
    total = unit(rrecv, 0, HALF)[...]
    for k in range(1, 2 * COLUMNS):
        total = total + unit(rrecv, k, HALF)[...]
    fsend[:TILES, :] = total / total[TILES - 1 : TILES, 127:128]

    def f_copy(to_col):
        return remote(unit(fsend, 0), unit(frecv, me), f_ss, f_rs, mine, to_col)

    for to_col in EARLY_COLUMNS:
        @pl.when(jnp.logical_or(mine != me, col != to_col))
        def _(to_col=to_col):
            f_copy(to_col).start()

    @pl.when(mine == me)
    def _():
        unit(frecv, me)[...] = fsend[:TILES, :]

    wait_rows(grecv, (SECTIONS - 1) * 2 * TILES, g_rs)
    for j in range(BOARD_DEV):
        keep = live_s[j] > 0
        for t in range(TILES):
            size = 128 if t < TILES - 1 else LAST
            at = pl.ds(128 * t, size)
            first = (j % 2 * 2 + j // 2) * NODES * UNIT
            gap = grecv[pl.ds(first + t, NODES, stride=UNIT), :][:, :size]
            stop = regret_v[0, j, :, at]
            go = regret_v[1, j, :, at]
            total_regret = stop + go
            out_stop[j, :, at] = jnp.where(keep, jnp.maximum(stop + go / total_regret * gap, 0.0), stop)
            out_go[j, :, at] = jnp.where(keep, jnp.maximum(go - stop / total_regret * gap, 0.0), go)

    wait_rows(asend, (SECTIONS - 1) * 2 * TILES, a_ss)
    wait_rows(gsend, (SECTIONS - 1) * 2 * TILES, g_ss)
    wait_rows(rsend, (2 * COLUMNS - 1) * TILES, r_ss)

    @pl.when(mine != me)
    def _():
        wait_rows(frecv, COLUMNS * TILES, f_ss)

    @pl.when(mine == me)
    def _():
        wait_rows(frecv, (COLUMNS - 1) * TILES, f_ss)

    @pl.when(mine != me)
    def _():
        wait_rows(frecv, SECTIONS * TILES, f_rs)

    @pl.when(mine == me)
    def _():
        wait_rows(frecv, (SECTIONS - 1) * TILES, f_rs)

    for p in range(2):
        for t in range(TILES):
            size = 128 if t < TILES - 1 else LAST
            tile = frecv[pl.ds(p * UNIT + t, NODES, stride=2 * UNIT), :]
            out_sec[p, :, pl.ds(128 * t, size)] = tile[:, :size]


def store(stop_v, go_v, sec_v, out_stop, out_go, out_sec, sem):
    pairs = ((stop_v, out_stop), (go_v, out_go), (sec_v, out_sec))
    copies = [pltpu.make_async_copy(src, dst.at[0], sem.at[i]) for i, (src, dst) in enumerate(pairs)]
    for copy in copies:
        copy.start()
    for copy in copies:
        copy.wait()


def local(root_reach, frontier_value, regret_stop, regret_go, board_live, board_cards, hand_rank):
    bits, scan = hand_bits()
    f32, i32 = jnp.float32, jnp.int32
    regrets = (BOARD_DEV, NODES, H)
    ends = (2, NODES, H)
    hbm_spec = pl.BlockSpec(memory_space=pltpu.HBM)
    vmem_spec = pl.BlockSpec(memory_space=pltpu.VMEM)
    dma = pltpu.SemaphoreType.DMA
    operands = (
        root_reach, frontier_value, regret_stop[0], regret_go[0], board_live, board_cards, hand_rank,
        jnp.asarray(bits), jnp.asarray(scan),
    )
    new_stop, new_go, section_value = pl.pallas_call(
        kernel,
        out_shape=(
            pltpu.VMEM(regrets, f32),
            pltpu.VMEM(regrets, f32),
            pltpu.VMEM(ends, f32),
        ),
        in_specs=[hbm_spec] * 9,
        out_specs=(vmem_spec,) * 3,
        scratch_shapes=[
            pltpu.VMEM(ends, f32), pltpu.VMEM(ends, f32), pltpu.VMEM((2, *regrets), f32),
            pltpu.SMEM((BOARD_DEV,), i32), pltpu.SMEM((BOARD_DEV, 5), i32), pltpu.VMEM((BOARD_DEV, H), i32),
            pltpu.VMEM((2, HP), i32), pltpu.VMEM((2, TILES, 128), i32),
            pltpu.VMEM((BOARD_DEV, NODES, 128), f32),
            pltpu.VMEM((2 * SECTIONS * UNIT, 128), f32), pltpu.VMEM((2 * SECTIONS * UNIT, 128), f32),
            pltpu.VMEM((4 * NODES * UNIT, 128), f32),
            pltpu.VMEM((8, HP), i32), pltpu.VMEM((8, HP), f32), pltpu.VMEM((2, 8, HP), i32), pltpu.VMEM((2, 8, HP), f32),
            pltpu.VMEM((HP, 8), i32), pltpu.VMEM((HP, 8), f32),
            pltpu.VMEM((2, HP, HP), jnp.bfloat16),
            pltpu.VMEM((4 * SECTIONS * UNIT, 128), f32), pltpu.VMEM((2, 2 * SECTIONS, HP), jnp.bfloat16),
            pltpu.VMEM((4 * SECTIONS * UNIT, 128), f32),
            pltpu.VMEM((2 * SECTIONS * UNIT, 128), f32), pltpu.VMEM((2 * SECTIONS * UNIT, 128), f32),
            pltpu.VMEM((2 * SECTIONS * HALF, 128), f32), pltpu.VMEM((2 * COLUMNS * HALF, 128), f32),
            pltpu.VMEM((HALF, 128), f32), pltpu.VMEM((SECTIONS * UNIT, 128), f32),
            dma((7,)), dma, dma, dma((2,)), *([dma] * 6),
        ],
        compiler_params=pltpu.CompilerParams(
            collective_id=0, has_side_effects=True, vmem_limit_bytes=32 * 1024 * 1024
        ),
    )(*(pltpu.with_memory_space_constraint(x, pltpu.HBM) for x in operands))
    return pl.pallas_call(
        store,
        out_shape=(
            jax.ShapeDtypeStruct((1, *regrets), f32),
            jax.ShapeDtypeStruct((1, *regrets), f32),
            jax.ShapeDtypeStruct((1, *ends), f32),
        ),
        in_specs=[vmem_spec] * 3,
        out_specs=(hbm_spec,) * 3,
        scratch_shapes=[dma((3,))],
        compiler_params=pltpu.CompilerParams(vmem_limit_bytes=1024 * 1024),
    )(new_stop, new_go, section_value)


def solution(mesh):
    regrets = P("section", "board", None, None)
    return jax.shard_map(
        local,
        mesh=mesh,
        in_specs=(P(), P(), regrets, regrets, P("board"), P("board", None), P("board", None)),
        out_specs=(regrets, regrets, P("section", None, None, None)),
        check_vma=False,
    )
```

```python
import jax
import jax.numpy as jnp
import numpy as np
from jax import lax
from jax.experimental import pallas as pl
from jax.experimental.pallas import tpu as pltpu
from jax.sharding import PartitionSpec as P

CARDS = 52
H = 1326
NODES = 8
TILES = 11
HP = TILES * 128
LAST = H - 128 * (TILES - 1)
SECTIONS = 16
COLUMNS = 16
BOARD_DEV = 4
UNIT = 24
BLOCK = 64
AHEAD = 2
HALF = 16
MESH = pl.DeviceIdType.MESH
ORDER = sorted(range(1, SECTIONS), key=lambda d: -min(d, SECTIONS - d))
EARLY_SECTIONS = (1, 3, 2, 0, 5, 4, 7, 6, 10, 11, 12, 13, 14, 15, 8, 9)
EARLY_COLUMNS = (0, 1, 3, 4, 2, 8, 5, 12, 7, 9, 6, 13, 11, 15, 10, 14)
FAR = sorted(range(COLUMNS), key=lambda d: -min(d // 4, 4 - d // 4) - min(d % 4, 4 - d % 4))


def hand_bits():
    first, second = np.triu_indices(CARDS, 1)
    low = np.full((HP,), -1, np.int64)
    high = np.full((HP,), -1, np.int64)
    both = (np.int64(1) << first) | (np.int64(1) << second)
    low[:H] = both & 0xFFFFFFFF
    high[:H] = both >> 32
    rows = np.stack([low, high]).astype(np.uint32).view(np.int32)
    return rows, rows.reshape(2, TILES, 128)


def remote(src, dst, send, recv, section, board):
    return pltpu.make_async_remote_copy(
        src_ref=src,
        dst_ref=dst,
        send_sem=send,
        recv_sem=recv,
        device_id={"section": section, "board": board},
        device_id_type=MESH,
    )


def unit(ref, index, stride=UNIT):
    return ref.at[pl.ds(pl.multiple_of(index * stride, 8), TILES), :]


def wait_rows(ref, rows, sem):
    some = ref.at[pl.ds(0, rows), :]
    pltpu.make_async_copy(some, some, sem).wait()


def kernel(
    root_hbm, front_hbm, stop_hbm, go_hbm, live_hbm, cards_hbm, rank_hbm, bits_hbm, scan_hbm,
    out_stop, out_go, out_sec,
    root_v, front_v, regret_v, live_s, cards_s, rank_v, bits_v, scan_v,
    pad, asend, arecv, ends, bitrow, rankrow, bitwide, rankwide, bitcol, rankcol, w, lsc, lhs, leafsc,
    gsend, grecv, rsend, rrecv, fsend, frecv,
    in_sem, regret_sem, a_ss, a_rs, g_ss, g_rs, r_ss, r_rs, f_ss, f_rs,
):
    me = lax.axis_index("section")
    col = lax.axis_index("board")
    node = me // 2
    core = me % 2
    row, lane = col // 4, col % 4

    def column(db):
        return (row + db // 4) % 4 * 4 + (lane + db % 4) % 4

    for i, src in enumerate((stop_hbm, go_hbm)):
        pltpu.make_async_copy(src, regret_v.at[i], regret_sem).start()

    barrier = pltpu.get_barrier_semaphore()

    def greet(section, board):
        pl.semaphore_signal(barrier, inc=1, device_id={"section": section, "board": board}, device_id_type=MESH)

    for d in ORDER:
        greet((me + d) % SECTIONS, col)
    loads = [
        pltpu.make_async_copy(src, dst, in_sem.at[i])
        for i, (src, dst) in enumerate(
            [
                (root_hbm, root_v), (front_hbm, front_v),
                (live_hbm, live_s), (cards_hbm, cards_s), (rank_hbm, rank_v), (bits_hbm, bits_v),
                (scan_hbm, scan_v),
            ]
        )
    ]
    for copy in loads:
        copy.start()
    for db in FAR[:-1]:
        for dc in range(2):
            greet(2 * node + (core + dc) % 2, column(db))
    pad[...] = jnp.full(pad.shape, 0.5, jnp.float32)
    ends[...] = jnp.zeros(ends.shape, jnp.float32)
    pltpu.make_async_copy(regret_v, regret_v, regret_sem).wait()

    for j in range(BOARD_DEV):
        for t in range(TILES):
            if t < TILES - 1:
                at = pl.ds(128 * t, 128)
                tile = regret_v[1, j, :, at] / (regret_v[1, j, :, at] + regret_v[0, j, :, at])
            else:
                at = pl.ds(128 * t, LAST)
                pad[j, :, :LAST] = regret_v[1, j, :, at] / (regret_v[1, j, :, at] + regret_v[0, j, :, at])
                tile = pad[j]
            first = (j % 2 * 2 + j // 2) * NODES * UNIT
            asend[pl.ds(first + t, NODES, stride=UNIT), :] = tile
    for copy in loads:
        copy.wait()

    alive = []
    board_bits = []
    for jj in range(2):
        j = 2 * core + jj
        alive.append(jnp.where(live_s[j] > 0, 1.0, 0.0).astype(jnp.float32))
        low = jnp.int32(0)
        high = jnp.int32(0)
        for i in range(5):
            card = cards_s[j, i]
            bit = lax.shift_left(jnp.int32(1), card % 32)
            low = low | jnp.where(card < 32, bit, 0)
            high = high | jnp.where(card < 32, 0, bit)
        board_bits.append((low, high))
    inside = (scan_v[0] & scan_v[1]) != -1
    mask = [
        jnp.where(((scan_v[0] & low) | (scan_v[1] & high)) == 0, 1.0, 0.0).astype(jnp.float32)
        for low, high in board_bits
    ]

    for which, ref in enumerate((root_v, front_v)):
        for p in range(2):
            base = (2 * which + p) * NODES * UNIT
            pad[p, :, :] = jnp.zeros((NODES, 128), jnp.float32)
            pad[p, :, :LAST] = ref[p, :, pl.ds(128 * (TILES - 1), LAST)]
            for t in range(TILES):
                tile = ref[p, :, pl.ds(128 * t, 128)] if t < TILES - 1 else pad[p]
                ends[pl.ds(base + t, NODES, stride=UNIT), :] = tile

    def end_of(index, jj):
        return unit(ends, index * NODES + node)[...] * mask[jj]

    bitrow[...] = jnp.zeros(bitrow.shape, jnp.int32)
    bitrow[0:2, :] = bits_v[...]
    rankrow[...] = jnp.zeros(rankrow.shape, jnp.float32)
    for jj in range(2):
        rankrow[jj : jj + 1, :H] = rank_v[pl.ds(2 * core + jj, 1), :].astype(jnp.float32)
    for r in range(2):
        bitwide[r] = jnp.broadcast_to(bitrow[r : r + 1, :], (8, HP))
        rankwide[r] = jnp.broadcast_to(rankrow[r : r + 1, :], (8, HP))
    for t in range(TILES):
        lanes = slice(128 * t, 128 * (t + 1))
        bitcol[lanes, :] = bitrow[:, lanes].T
        rankcol[lanes, :] = rankrow[:, lanes].T

    def payoff_rows(block, _):
        at = [pl.multiple_of(block * BLOCK + 16 * i, 16) for i in range(BLOCK // 16)]
        wide = [
            [jnp.broadcast_to(ref[pl.ds(a, 16), r : r + 1], (16, 128)) for ref in (bitcol, rankcol) for r in range(2)]
            for a in at
        ]
        one = jnp.bfloat16(1)
        for t in range(TILES):
            lanes = slice(128 * t, 128 * (t + 1))
            low, high, rank0, rank1 = (
                jnp.concatenate([ref[r, :, lanes]] * 2, axis=0) for ref in (bitwide, rankwide) for r in range(2)
            )
            for a, (low_g, high_g, rank0_g, rank1_g) in zip(at, wide):
                shared = (low_g & low) | (high_g & high)
                free = jnp.where(shared == 0, 1.0, 0.0).astype(jnp.bfloat16)
                for jj, step in enumerate((rank0 - rank0_g, rank1 - rank1_g)):
                    step = step.astype(jnp.bfloat16)
                    w[jj, pl.ds(a, 16), lanes] = jnp.minimum(jnp.maximum(step, -one), one) * free
        return 0

    lax.fori_loop(0, AHEAD, payoff_rows, 0)
    pl.semaphore_wait(barrier, SECTIONS - 1 + 2 * (COLUMNS - 1))

    def a_unit(jj, to):
        return (2 * jj + to % 2) * NODES + to // 2

    def a_copy(jj, to):
        return remote(
            unit(asend, a_unit(jj, to)), unit(arecv, jj * SECTIONS + me), a_ss, a_rs.at[jj], to, col
        )

    for jj in range(2):
        for d in ORDER:
            a_copy(jj, (me + d) % SECTIONS).start()
    for jj in range(2):
        unit(arecv, jj * SECTIONS + me)[...] = unit(asend, a_unit(jj, me))[...]

    lax.fori_loop(AHEAD, HP // BLOCK, payoff_rows, 0)

    for jj in range(2):
        wait_rows(arecv, (SECTIONS - 1) * TILES, a_rs.at[jj])
        reach = [end_of(0, jj), end_of(1, jj)]
        for s in range(SECTIONS):
            go = jnp.where(inside, unit(arecv, jj * SECTIONS + s)[...], 0.5)
            q = s % 2
            unit(lsc, (2 * jj + q) * SECTIONS + s)[...] = reach[q] * (1.0 - go)
            unit(lsc, (2 * jj + 1 - q) * SECTIONS + s)[...] = reach[1 - q]
            reach[q] = reach[q] * go
        for p in range(2):
            for t in range(TILES):
                tile = lsc[pl.ds((2 * jj + p) * SECTIONS * UNIT + t, SECTIONS, stride=UNIT), :]
                lhs[jj, p * SECTIONS : (p + 1) * SECTIONS, 128 * t : 128 * (t + 1)] = tile.astype(jnp.bfloat16)
        leaf = jnp.dot(lhs[jj], w[jj], preferred_element_type=jnp.float32)
        for p in range(2):
            for t in range(TILES):
                tile = leaf[p * SECTIONS : (p + 1) * SECTIONS, 128 * t : 128 * (t + 1)]
                leafsc[pl.ds((2 * jj + 1 - p) * SECTIONS * UNIT + t, SECTIONS, stride=UNIT), :] = tile

    value = [[end_of(2, jj), end_of(3, jj)] for jj in range(2)]
    for s in reversed(range(SECTIONS)):
        q = s % 2
        for jj in range(2):
            go = jnp.where(inside, unit(arecv, jj * SECTIONS + s)[...], 0.5)
            leaf_q = unit(leafsc, (2 * jj + q) * SECTIONS + s)[...] * mask[jj]
            leaf_o = unit(leafsc, (2 * jj + 1 - q) * SECTIONS + s)[...] * mask[jj]
            gsend[s * UNIT + jj * TILES : s * UNIT + (jj + 1) * TILES, :] = leaf_q - value[jj][q]
            value[jj][q] = (1.0 - go) * leaf_q + go * value[jj][q]
            value[jj][1 - q] = leaf_o + value[jj][1 - q]
        for p in range(2):
            unit(rsend, 2 * s + p, HALF)[...] = sum(
                jnp.where(inside, value[jj][p], 1.0) * alive[jj] for jj in range(2)
            )

    mine = (col + 7 * me) % SECTIONS

    def r_copy(s, p):
        to = 2 * node + p
        return remote(
            unit(rsend, 2 * s + p, HALF), unit(rrecv, core * COLUMNS + col, HALF), r_ss, r_rs,
            to, (s + (SECTIONS - 7) * to) % COLUMNS,
        )

    for s in EARLY_SECTIONS:
        for p in range(2):
            @pl.when(jnp.logical_or(core != p, mine != s))
            def _(s=s, p=p):
                r_copy(s, p).start()

    unit(rrecv, core * COLUMNS + col, HALF)[...] = unit(rsend, 2 * mine + core, HALF)[...]

    def block(ref, index):
        return ref.at[pl.ds(pl.multiple_of(index * UNIT, 8), 2 * TILES), :]

    def place(to):
        return to % 2 * NODES + to // 2

    def g_copy(to):
        return remote(block(gsend, to), block(grecv, place(me)), g_ss, g_rs, to, col)

    for d in ORDER:
        g_copy((me + d) % SECTIONS).start()
    block(grecv, place(me))[...] = block(gsend, me)[...]

    wait_rows(rrecv, (2 * COLUMNS - 1) * TILES, r_rs)
    sums = [unit(rrecv, k, HALF)[...] for k in range(4)]
    for k in range(4, 2 * COLUMNS):
        sums[k % 4] = sums[k % 4] + unit(rrecv, k, HALF)[...]
    total = (sums[0] + sums[1]) + (sums[2] + sums[3])
    fsend[:TILES, :] = total / total[TILES - 1 : TILES, 127:128]

    def f_copy(to_col):
        return remote(unit(fsend, 0), unit(frecv, me), f_ss, f_rs, mine, to_col)

    for to_col in EARLY_COLUMNS:
        @pl.when(jnp.logical_or(mine != me, col != to_col))
        def _(to_col=to_col):
            f_copy(to_col).start()

    @pl.when(mine == me)
    def _():
        unit(frecv, me)[...] = fsend[:TILES, :]

    wait_rows(grecv, (SECTIONS - 1) * 2 * TILES, g_rs)
    for j in range(BOARD_DEV):
        keep = live_s[j] > 0
        for t in range(TILES):
            size = 128 if t < TILES - 1 else LAST
            at = pl.ds(128 * t, size)
            first = j // 2 * NODES * UNIT + j % 2 * TILES
            gap = grecv[pl.ds(first + t, NODES, stride=UNIT), :][:, :size]
            stop = regret_v[0, j, :, at]
            go = regret_v[1, j, :, at]
            total_regret = stop + go
            out_stop[j, :, at] = jnp.where(keep, jnp.maximum(stop + go / total_regret * gap, 0.0), stop)
            out_go[j, :, at] = jnp.where(keep, jnp.maximum(go - stop / total_regret * gap, 0.0), go)

    wait_rows(asend, (SECTIONS - 1) * 2 * TILES, a_ss)
    wait_rows(gsend, (SECTIONS - 1) * 2 * TILES, g_ss)
    wait_rows(rsend, (2 * COLUMNS - 1) * TILES, r_ss)

    @pl.when(mine != me)
    def _():
        wait_rows(frecv, COLUMNS * TILES, f_ss)

    @pl.when(mine == me)
    def _():
        wait_rows(frecv, (COLUMNS - 1) * TILES, f_ss)

    @pl.when(mine != me)
    def _():
        wait_rows(frecv, SECTIONS * TILES, f_rs)

    @pl.when(mine == me)
    def _():
        wait_rows(frecv, (SECTIONS - 1) * TILES, f_rs)

    for p in range(2):
        for t in range(TILES):
            size = 128 if t < TILES - 1 else LAST
            tile = frecv[pl.ds(p * UNIT + t, NODES, stride=2 * UNIT), :]
            out_sec[p, :, pl.ds(128 * t, size)] = tile[:, :size]


def store(stop_v, go_v, sec_v, out_stop, out_go, out_sec, sem):
    pairs = ((stop_v, out_stop), (go_v, out_go), (sec_v, out_sec))
    copies = [pltpu.make_async_copy(src, dst.at[0], sem.at[i]) for i, (src, dst) in enumerate(pairs)]
    for copy in copies:
        copy.start()
    for copy in copies:
        copy.wait()


def local(root_reach, frontier_value, regret_stop, regret_go, board_live, board_cards, hand_rank):
    bits, scan = hand_bits()
    f32, i32 = jnp.float32, jnp.int32
    regrets = (BOARD_DEV, NODES, H)
    ends = (2, NODES, H)
    hbm_spec = pl.BlockSpec(memory_space=pltpu.HBM)
    vmem_spec = pl.BlockSpec(memory_space=pltpu.VMEM)
    dma = pltpu.SemaphoreType.DMA
    operands = (
        root_reach, frontier_value, regret_stop[0], regret_go[0], board_live, board_cards, hand_rank,
        jnp.asarray(bits), jnp.asarray(scan),
    )
    new_stop, new_go, section_value = pl.pallas_call(
        kernel,
        out_shape=(
            pltpu.VMEM(regrets, f32),
            pltpu.VMEM(regrets, f32),
            pltpu.VMEM(ends, f32),
        ),
        in_specs=[hbm_spec] * 9,
        out_specs=(vmem_spec,) * 3,
        scratch_shapes=[
            pltpu.VMEM(ends, f32), pltpu.VMEM(ends, f32), pltpu.VMEM((2, *regrets), f32),
            pltpu.SMEM((BOARD_DEV,), i32), pltpu.SMEM((BOARD_DEV, 5), i32), pltpu.VMEM((BOARD_DEV, H), i32),
            pltpu.VMEM((2, HP), i32), pltpu.VMEM((2, TILES, 128), i32),
            pltpu.VMEM((BOARD_DEV, NODES, 128), f32),
            pltpu.VMEM((2 * SECTIONS * UNIT, 128), f32), pltpu.VMEM((2 * SECTIONS * UNIT, 128), f32),
            pltpu.VMEM((4 * NODES * UNIT, 128), f32),
            pltpu.VMEM((8, HP), i32), pltpu.VMEM((8, HP), f32), pltpu.VMEM((2, 8, HP), i32), pltpu.VMEM((2, 8, HP), f32),
            pltpu.VMEM((HP, 8), i32), pltpu.VMEM((HP, 8), f32),
            pltpu.VMEM((2, HP, HP), jnp.bfloat16),
            pltpu.VMEM((4 * SECTIONS * UNIT, 128), f32), pltpu.VMEM((2, 2 * SECTIONS, HP), jnp.bfloat16),
            pltpu.VMEM((4 * SECTIONS * UNIT, 128), f32),
            pltpu.VMEM((SECTIONS * UNIT, 128), f32), pltpu.VMEM((SECTIONS * UNIT, 128), f32),
            pltpu.VMEM((2 * SECTIONS * HALF, 128), f32), pltpu.VMEM((2 * COLUMNS * HALF, 128), f32),
            pltpu.VMEM((HALF, 128), f32), pltpu.VMEM((SECTIONS * UNIT, 128), f32),
            dma((7,)), dma, dma, dma((2,)), *([dma] * 6),
        ],
        compiler_params=pltpu.CompilerParams(
            collective_id=0, has_side_effects=True, vmem_limit_bytes=32 * 1024 * 1024
        ),
    )(*(pltpu.with_memory_space_constraint(x, pltpu.HBM) for x in operands))
    return pl.pallas_call(
        store,
        out_shape=(
            jax.ShapeDtypeStruct((1, *regrets), f32),
            jax.ShapeDtypeStruct((1, *regrets), f32),
            jax.ShapeDtypeStruct((1, *ends), f32),
        ),
        in_specs=[vmem_spec] * 3,
        out_specs=(hbm_spec,) * 3,
        scratch_shapes=[dma((3,))],
        compiler_params=pltpu.CompilerParams(vmem_limit_bytes=1024 * 1024),
    )(new_stop, new_go, section_value)


def solution(mesh):
    regrets = P("section", "board", None, None)
    return jax.shard_map(
        local,
        mesh=mesh,
        in_specs=(P(), P(), regrets, regrets, P("board"), P("board", None), P("board", None)),
        out_specs=(regrets, regrets, P("section", None, None, None)),
        check_vma=False,
    )
```

```python
import jax
import jax.numpy as jnp
import numpy as np
from jax import lax
from jax.experimental import pallas as pl
from jax.experimental.pallas import tpu as pltpu
from jax.sharding import PartitionSpec as P

CARDS = 52
H = 1326
NODES = 8
TILES = 11
HP = TILES * 128
LAST = H - 128 * (TILES - 1)
SECTIONS = 16
COLUMNS = 16
BOARD_DEV = 4
UNIT = 24
BLOCK = 64
AHEAD = 2
HALF = 16
MESH = pl.DeviceIdType.MESH
ORDER = sorted(range(1, SECTIONS), key=lambda d: -min(d, SECTIONS - d))
EARLY_SECTIONS = (1, 3, 2, 0, 5, 4, 7, 6, 10, 11, 12, 13, 14, 15, 8, 9)
EARLY_COLUMNS = (0, 1, 3, 4, 2, 8, 5, 12, 7, 9, 6, 13, 11, 15, 10, 14)
FAR = sorted(range(COLUMNS), key=lambda d: -min(d // 4, 4 - d // 4) - min(d % 4, 4 - d % 4))


def hand_bits():
    first, second = np.triu_indices(CARDS, 1)
    low = np.full((HP,), -1, np.int64)
    high = np.full((HP,), -1, np.int64)
    both = (np.int64(1) << first) | (np.int64(1) << second)
    low[:H] = both & 0xFFFFFFFF
    high[:H] = both >> 32
    rows = np.stack([low, high]).astype(np.uint32).view(np.int32)
    return rows, rows.reshape(2, TILES, 128)


def remote(src, dst, send, recv, section, board):
    return pltpu.make_async_remote_copy(
        src_ref=src,
        dst_ref=dst,
        send_sem=send,
        recv_sem=recv,
        device_id={"section": section, "board": board},
        device_id_type=MESH,
    )


def unit(ref, index, stride=UNIT):
    return ref.at[pl.ds(pl.multiple_of(index * stride, 8), TILES), :]


def wait_rows(ref, rows, sem):
    some = ref.at[pl.ds(0, rows), :]
    pltpu.make_async_copy(some, some, sem).wait()


def kernel(
    root_hbm, front_hbm, stop_hbm, go_hbm, live_hbm, cards_hbm, rank_hbm, bits_hbm, scan_hbm,
    out_stop, out_go, out_sec,
    root_v, front_v, regret_v, live_s, cards_s, rank_v, bits_v, scan_v,
    pad, asend, arecv, ends, bitrow, rankrow, bitwide, rankwide, bitcol, rankcol, w, lsc, lhs, leafsc,
    gsend, grecv, rsend, rrecv, fsend, frecv,
    in_sem, regret_sem, a_ss, a_rs, g_ss, g_rs, r_ss, r_rs, f_ss, f_rs,
):
    me = lax.axis_index("section")
    col = lax.axis_index("board")
    node = me // 2
    core = me % 2
    row, lane = col // 4, col % 4

    def column(db):
        return (row + db // 4) % 4 * 4 + (lane + db % 4) % 4

    for i, src in enumerate((stop_hbm, go_hbm)):
        pltpu.make_async_copy(src, regret_v.at[i], regret_sem).start()

    barrier = pltpu.get_barrier_semaphore()

    def greet(section, board):
        pl.semaphore_signal(barrier, inc=1, device_id={"section": section, "board": board}, device_id_type=MESH)

    for d in ORDER:
        greet((me + d) % SECTIONS, col)
    loads = [
        pltpu.make_async_copy(src, dst, in_sem.at[i])
        for i, (src, dst) in enumerate(
            [
                (root_hbm, root_v), (front_hbm, front_v),
                (live_hbm, live_s), (cards_hbm, cards_s), (rank_hbm, rank_v), (bits_hbm, bits_v),
                (scan_hbm, scan_v),
            ]
        )
    ]
    for copy in loads:
        copy.start()
    for db in FAR[:-1]:
        for dc in range(2):
            greet(2 * node + (core + dc) % 2, column(db))
    pad[...] = jnp.full(pad.shape, 0.5, jnp.float32)
    ends[...] = jnp.zeros(ends.shape, jnp.float32)
    pltpu.make_async_copy(regret_v, regret_v, regret_sem).wait()

    for j in range(BOARD_DEV):
        for t in range(TILES):
            if t < TILES - 1:
                at = pl.ds(128 * t, 128)
                tile = regret_v[1, j, :, at] / (regret_v[1, j, :, at] + regret_v[0, j, :, at])
            else:
                at = pl.ds(128 * t, LAST)
                pad[j, :, :LAST] = regret_v[1, j, :, at] / (regret_v[1, j, :, at] + regret_v[0, j, :, at])
                tile = pad[j]
            first = (j % 2 * 2 + j // 2) * NODES * UNIT
            asend[pl.ds(first + t, NODES, stride=UNIT), :] = tile
    for copy in loads:
        copy.wait()

    alive = []
    board_bits = []
    for jj in range(2):
        j = 2 * core + jj
        alive.append(jnp.where(live_s[j] > 0, 1.0, 0.0).astype(jnp.float32))
        low = jnp.int32(0)
        high = jnp.int32(0)
        for i in range(5):
            card = cards_s[j, i]
            bit = lax.shift_left(jnp.int32(1), card % 32)
            low = low | jnp.where(card < 32, bit, 0)
            high = high | jnp.where(card < 32, 0, bit)
        board_bits.append((low, high))
    inside = (scan_v[0] & scan_v[1]) != -1
    mask = [
        jnp.where(((scan_v[0] & low) | (scan_v[1] & high)) == 0, 1.0, 0.0).astype(jnp.float32)
        for low, high in board_bits
    ]

    for which, ref in enumerate((root_v, front_v)):
        for p in range(2):
            base = (2 * which + p) * NODES * UNIT
            pad[p, :, :] = jnp.zeros((NODES, 128), jnp.float32)
            pad[p, :, :LAST] = ref[p, :, pl.ds(128 * (TILES - 1), LAST)]
            for t in range(TILES):
                tile = ref[p, :, pl.ds(128 * t, 128)] if t < TILES - 1 else pad[p]
                ends[pl.ds(base + t, NODES, stride=UNIT), :] = tile

    def end_of(index, jj):
        return unit(ends, index * NODES + node)[...] * mask[jj]

    bitrow[...] = jnp.zeros(bitrow.shape, jnp.int32)
    bitrow[0:2, :] = bits_v[...]
    rankrow[...] = jnp.zeros(rankrow.shape, jnp.float32)
    for jj in range(2):
        rankrow[jj : jj + 1, :H] = rank_v[pl.ds(2 * core + jj, 1), :].astype(jnp.float32)
    for r in range(2):
        bitwide[r] = jnp.broadcast_to(bitrow[r : r + 1, :], (8, HP))
        rankwide[r] = jnp.broadcast_to(rankrow[r : r + 1, :], (8, HP))
    for t in range(TILES):
        lanes = slice(128 * t, 128 * (t + 1))
        bitcol[lanes, :] = bitrow[:, lanes].T
        rankcol[lanes, :] = rankrow[:, lanes].T

    def payoff_rows(block, _):
        at = [pl.multiple_of(block * BLOCK + 16 * i, 16) for i in range(BLOCK // 16)]
        wide = [
            [jnp.broadcast_to(ref[pl.ds(a, 16), r : r + 1], (16, 128)) for ref in (bitcol, rankcol) for r in range(2)]
            for a in at
        ]
        one = jnp.bfloat16(1)
        for t in range(TILES):
            lanes = slice(128 * t, 128 * (t + 1))
            low, high, rank0, rank1 = (
                jnp.concatenate([ref[r, :, lanes]] * 2, axis=0) for ref in (bitwide, rankwide) for r in range(2)
            )
            for a, (low_g, high_g, rank0_g, rank1_g) in zip(at, wide):
                shared = (low_g & low) | (high_g & high)
                free = jnp.where(shared == 0, 1.0, 0.0).astype(jnp.bfloat16)
                for jj, step in enumerate((rank0 - rank0_g, rank1 - rank1_g)):
                    step = step.astype(jnp.bfloat16)
                    w[jj, pl.ds(a, 16), lanes] = jnp.minimum(jnp.maximum(step, -one), one) * free
        return 0

    lax.fori_loop(0, AHEAD, payoff_rows, 0)
    pl.semaphore_wait(barrier, SECTIONS - 1 + 2 * (COLUMNS - 1))

    def a_unit(jj, to):
        return (2 * jj + to % 2) * NODES + to // 2

    def a_copy(jj, to):
        return remote(
            unit(asend, a_unit(jj, to)), unit(arecv, jj * SECTIONS + me), a_ss, a_rs.at[jj], to, col
        )

    for jj in range(2):
        for d in ORDER:
            a_copy(jj, (me + d) % SECTIONS).start()
    for jj in range(2):
        unit(arecv, jj * SECTIONS + me)[...] = unit(asend, a_unit(jj, me))[...]

    lax.fori_loop(AHEAD, HP // BLOCK, payoff_rows, 0)

    for jj in range(2):
        wait_rows(arecv, (SECTIONS - 1) * TILES, a_rs.at[jj])
        reach = [end_of(0, jj), end_of(1, jj)]
        for s in range(SECTIONS):
            go = jnp.where(inside, unit(arecv, jj * SECTIONS + s)[...], 0.5)
            q = s % 2
            unit(lsc, (2 * jj + q) * SECTIONS + s)[...] = reach[q] * (1.0 - go)
            unit(lsc, (2 * jj + 1 - q) * SECTIONS + s)[...] = reach[1 - q]
            reach[q] = reach[q] * go
        for p in range(2):
            for t in range(TILES):
                tile = lsc[pl.ds((2 * jj + p) * SECTIONS * UNIT + t, SECTIONS, stride=UNIT), :]
                lhs[jj, p * SECTIONS : (p + 1) * SECTIONS, 128 * t : 128 * (t + 1)] = tile.astype(jnp.bfloat16)
        leaf = jnp.dot(lhs[jj], w[jj], preferred_element_type=jnp.float32)
        for p in range(2):
            for t in range(TILES):
                tile = leaf[p * SECTIONS : (p + 1) * SECTIONS, 128 * t : 128 * (t + 1)]
                leafsc[pl.ds((2 * jj + 1 - p) * SECTIONS * UNIT + t, SECTIONS, stride=UNIT), :] = tile
        value = [end_of(2, jj), end_of(3, jj)]
        for s in reversed(range(SECTIONS)):
            q = s % 2
            go = jnp.where(inside, unit(arecv, jj * SECTIONS + s)[...], 0.5)
            leaf_q = unit(leafsc, (2 * jj + q) * SECTIONS + s)[...] * mask[jj]
            leaf_o = unit(leafsc, (2 * jj + 1 - q) * SECTIONS + s)[...] * mask[jj]
            gsend[s * UNIT + jj * TILES : s * UNIT + (jj + 1) * TILES, :] = leaf_q - value[q]
            value[q] = (1.0 - go) * leaf_q + go * value[q]
            value[1 - q] = leaf_o + value[1 - q]
            for p in range(2):
                row = unit(rsend, 2 * s + p, HALF)
                part = jnp.where(inside, value[p], 1.0) * alive[jj]
                row[...] = part if jj == 0 else row[...] + part

    mine = (col + 7 * me) % SECTIONS

    def r_copy(s, p):
        to = 2 * node + p
        return remote(
            unit(rsend, 2 * s + p, HALF), unit(rrecv, core * COLUMNS + col, HALF), r_ss, r_rs,
            to, (s + (SECTIONS - 7) * to) % COLUMNS,
        )

    for s in EARLY_SECTIONS:
        for p in range(2):
            @pl.when(jnp.logical_or(core != p, mine != s))
            def _(s=s, p=p):
                r_copy(s, p).start()

    unit(rrecv, core * COLUMNS + col, HALF)[...] = unit(rsend, 2 * mine + core, HALF)[...]

    def block(ref, index):
        return ref.at[pl.ds(pl.multiple_of(index * UNIT, 8), 2 * TILES), :]

    def place(to):
        return to % 2 * NODES + to // 2

    def g_copy(to):
        return remote(block(gsend, to), block(grecv, place(me)), g_ss, g_rs, to, col)

    for d in ORDER:
        g_copy((me + d) % SECTIONS).start()
    block(grecv, place(me))[...] = block(gsend, me)[...]

    wait_rows(rrecv, (2 * COLUMNS - 1) * TILES, r_rs)
    sums = [unit(rrecv, k, HALF)[...] for k in range(4)]
    for k in range(4, 2 * COLUMNS):
        sums[k % 4] = sums[k % 4] + unit(rrecv, k, HALF)[...]
    total = (sums[0] + sums[1]) + (sums[2] + sums[3])
    fsend[:TILES, :] = total / total[TILES - 1 : TILES, 127:128]

    def f_copy(to_col):
        return remote(unit(fsend, 0), unit(frecv, me), f_ss, f_rs, mine, to_col)

    for to_col in EARLY_COLUMNS:
        @pl.when(jnp.logical_or(mine != me, col != to_col))
        def _(to_col=to_col):
            f_copy(to_col).start()

    @pl.when(mine == me)
    def _():
        unit(frecv, me)[...] = fsend[:TILES, :]

    wait_rows(grecv, (SECTIONS - 1) * 2 * TILES, g_rs)
    for j in range(BOARD_DEV):
        keep = live_s[j] > 0
        for t in range(TILES):
            size = 128 if t < TILES - 1 else LAST
            at = pl.ds(128 * t, size)
            first = j // 2 * NODES * UNIT + j % 2 * TILES
            gap = grecv[pl.ds(first + t, NODES, stride=UNIT), :][:, :size]
            stop = regret_v[0, j, :, at]
            go = regret_v[1, j, :, at]
            total_regret = stop + go
            out_stop[j, :, at] = jnp.where(keep, jnp.maximum(stop + go / total_regret * gap, 0.0), stop)
            out_go[j, :, at] = jnp.where(keep, jnp.maximum(go - stop / total_regret * gap, 0.0), go)

    wait_rows(asend, (SECTIONS - 1) * 2 * TILES, a_ss)
    wait_rows(gsend, (SECTIONS - 1) * 2 * TILES, g_ss)
    wait_rows(rsend, (2 * COLUMNS - 1) * TILES, r_ss)

    @pl.when(mine != me)
    def _():
        wait_rows(frecv, COLUMNS * TILES, f_ss)

    @pl.when(mine == me)
    def _():
        wait_rows(frecv, (COLUMNS - 1) * TILES, f_ss)

    @pl.when(mine != me)
    def _():
        wait_rows(frecv, SECTIONS * TILES, f_rs)

    @pl.when(mine == me)
    def _():
        wait_rows(frecv, (SECTIONS - 1) * TILES, f_rs)

    for p in range(2):
        for t in range(TILES):
            size = 128 if t < TILES - 1 else LAST
            tile = frecv[pl.ds(p * UNIT + t, NODES, stride=2 * UNIT), :]
            out_sec[p, :, pl.ds(128 * t, size)] = tile[:, :size]


def store(stop_v, go_v, sec_v, out_stop, out_go, out_sec, sem):
    pairs = ((stop_v, out_stop), (go_v, out_go), (sec_v, out_sec))
    copies = [pltpu.make_async_copy(src, dst.at[0], sem.at[i]) for i, (src, dst) in enumerate(pairs)]
    for copy in copies:
        copy.start()
    for copy in copies:
        copy.wait()


def local(root_reach, frontier_value, regret_stop, regret_go, board_live, board_cards, hand_rank):
    bits, scan = hand_bits()
    f32, i32 = jnp.float32, jnp.int32
    regrets = (BOARD_DEV, NODES, H)
    ends = (2, NODES, H)
    hbm_spec = pl.BlockSpec(memory_space=pltpu.HBM)
    vmem_spec = pl.BlockSpec(memory_space=pltpu.VMEM)
    dma = pltpu.SemaphoreType.DMA
    operands = (
        root_reach, frontier_value, regret_stop[0], regret_go[0], board_live, board_cards, hand_rank,
        jnp.asarray(bits), jnp.asarray(scan),
    )
    new_stop, new_go, section_value = pl.pallas_call(
        kernel,
        out_shape=(
            pltpu.VMEM(regrets, f32),
            pltpu.VMEM(regrets, f32),
            pltpu.VMEM(ends, f32),
        ),
        in_specs=[hbm_spec] * 9,
        out_specs=(vmem_spec,) * 3,
        scratch_shapes=[
            pltpu.VMEM(ends, f32), pltpu.VMEM(ends, f32), pltpu.VMEM((2, *regrets), f32),
            pltpu.SMEM((BOARD_DEV,), i32), pltpu.SMEM((BOARD_DEV, 5), i32), pltpu.VMEM((BOARD_DEV, H), i32),
            pltpu.VMEM((2, HP), i32), pltpu.VMEM((2, TILES, 128), i32),
            pltpu.VMEM((BOARD_DEV, NODES, 128), f32),
            pltpu.VMEM((2 * SECTIONS * UNIT, 128), f32), pltpu.VMEM((2 * SECTIONS * UNIT, 128), f32),
            pltpu.VMEM((4 * NODES * UNIT, 128), f32),
            pltpu.VMEM((8, HP), i32), pltpu.VMEM((8, HP), f32), pltpu.VMEM((2, 8, HP), i32), pltpu.VMEM((2, 8, HP), f32),
            pltpu.VMEM((HP, 8), i32), pltpu.VMEM((HP, 8), f32),
            pltpu.VMEM((2, HP, HP), jnp.bfloat16),
            pltpu.VMEM((4 * SECTIONS * UNIT, 128), f32), pltpu.VMEM((2, 2 * SECTIONS, HP), jnp.bfloat16),
            pltpu.VMEM((4 * SECTIONS * UNIT, 128), f32),
            pltpu.VMEM((SECTIONS * UNIT, 128), f32), pltpu.VMEM((SECTIONS * UNIT, 128), f32),
            pltpu.VMEM((2 * SECTIONS * HALF, 128), f32), pltpu.VMEM((2 * COLUMNS * HALF, 128), f32),
            pltpu.VMEM((HALF, 128), f32), pltpu.VMEM((SECTIONS * UNIT, 128), f32),
            dma((7,)), dma, dma, dma((2,)), *([dma] * 6),
        ],
        compiler_params=pltpu.CompilerParams(
            collective_id=0, has_side_effects=True, vmem_limit_bytes=32 * 1024 * 1024
        ),
    )(*(pltpu.with_memory_space_constraint(x, pltpu.HBM) for x in operands))
    return pl.pallas_call(
        store,
        out_shape=(
            jax.ShapeDtypeStruct((1, *regrets), f32),
            jax.ShapeDtypeStruct((1, *regrets), f32),
            jax.ShapeDtypeStruct((1, *ends), f32),
        ),
        in_specs=[vmem_spec] * 3,
        out_specs=(hbm_spec,) * 3,
        scratch_shapes=[dma((3,))],
        compiler_params=pltpu.CompilerParams(vmem_limit_bytes=1024 * 1024),
    )(new_stop, new_go, section_value)


def solution(mesh):
    regrets = P("section", "board", None, None)
    return jax.shard_map(
        local,
        mesh=mesh,
        in_specs=(P(), P(), regrets, regrets, P("board"), P("board", None), P("board", None)),
        out_specs=(regrets, regrets, P("section", None, None, None)),
        check_vma=False,
    )
```

```python
import jax
import jax.numpy as jnp
import numpy as np
from jax import lax
from jax.experimental import pallas as pl
from jax.experimental.pallas import tpu as pltpu
from jax.sharding import PartitionSpec as P

CARDS = 52
H = 1326
NODES = 8
TILES = 11
HP = TILES * 128
LAST = H - 128 * (TILES - 1)
SECTIONS = 16
COLUMNS = 16
BOARD_DEV = 4
UNIT = 24
BLOCK = 64
AHEAD = 2
HALF = 16
MESH = pl.DeviceIdType.MESH
ORDER = sorted(range(1, SECTIONS), key=lambda d: -min(d, SECTIONS - d))
EARLY_SECTIONS = (1, 3, 2, 0, 5, 4, 7, 6, 10, 11, 12, 13, 14, 15, 8, 9)
EARLY_COLUMNS = (0, 1, 3, 4, 2, 8, 5, 12, 7, 9, 6, 13, 11, 15, 10, 14)
def far_of(d):
    return min(d // 4, 4 - d // 4) + min(d % 4, 4 - d % 4)


FAR = sorted(range(COLUMNS), key=lambda d: -far_of(d))


def hand_bits():
    first, second = np.triu_indices(CARDS, 1)
    low = np.full((HP,), -1, np.int64)
    high = np.full((HP,), -1, np.int64)
    both = (np.int64(1) << first) | (np.int64(1) << second)
    low[:H] = both & 0xFFFFFFFF
    high[:H] = both >> 32
    rows = np.stack([low, high]).astype(np.uint32).view(np.int32)
    return rows, rows.reshape(2, TILES, 128)


def remote(src, dst, send, recv, section, board):
    return pltpu.make_async_remote_copy(
        src_ref=src,
        dst_ref=dst,
        send_sem=send,
        recv_sem=recv,
        device_id={"section": section, "board": board},
        device_id_type=MESH,
    )


def unit(ref, index, stride=UNIT):
    return ref.at[pl.ds(pl.multiple_of(index * stride, 8), TILES), :]


def wait_rows(ref, rows, sem):
    some = ref.at[pl.ds(0, rows), :]
    pltpu.make_async_copy(some, some, sem).wait()


def kernel(
    root_hbm, front_hbm, stop_hbm, go_hbm, live_hbm, cards_hbm, rank_hbm, bits_hbm, scan_hbm,
    out_stop, out_go, out_sec,
    root_v, front_v, regret_v, live_s, cards_s, rank_v, bits_v, scan_v,
    pad, asend, arecv, ends, bitrow, rankrow, bitwide, rankwide, bitcol, rankcol, w, lsc, lhs, leafsc,
    gsend, grecv, rsend, rrecv, fsend, frecv,
    in_sem, regret_sem, a_ss, a_rs, g_ss, g_rs, r_ss, r_rs, f_ss, f_rs,
):
    me = lax.axis_index("section")
    col = lax.axis_index("board")
    node = me // 2
    core = me % 2
    row, lane = col // 4, col % 4

    def column(db):
        return (row + db // 4) % 4 * 4 + (lane + db % 4) % 4

    for i, src in enumerate((stop_hbm, go_hbm)):
        pltpu.make_async_copy(src, regret_v.at[i], regret_sem).start()

    barrier = pltpu.get_barrier_semaphore()

    def greet(section, board):
        pl.semaphore_signal(barrier, inc=1, device_id={"section": section, "board": board}, device_id_type=MESH)

    def greet_all(near):
        for hops in (2, 1, 0) if near else (4, 3):
            for d in ORDER:
                if (min(d, SECTIONS - d) + 1) // 2 == hops or (hops == 0 and d == 0):
                    greet((me + d) % SECTIONS, col)
            for db in FAR[:-1]:
                if far_of(db) == hops:
                    for dc in range(2):
                        greet(2 * node + (core + dc) % 2, column(db))

    greet_all(False)
    loads = [
        pltpu.make_async_copy(src, dst, in_sem.at[i])
        for i, (src, dst) in enumerate(
            [
                (root_hbm, root_v), (front_hbm, front_v),
                (live_hbm, live_s), (cards_hbm, cards_s), (rank_hbm, rank_v), (bits_hbm, bits_v),
                (scan_hbm, scan_v),
            ]
        )
    ]
    for copy in loads:
        copy.start()
    greet_all(True)
    pad[...] = jnp.full(pad.shape, 0.5, jnp.float32)
    ends[...] = jnp.zeros(ends.shape, jnp.float32)
    pltpu.make_async_copy(regret_v, regret_v, regret_sem).wait()

    for j in range(BOARD_DEV):
        for t in range(TILES):
            if t < TILES - 1:
                at = pl.ds(128 * t, 128)
                tile = regret_v[1, j, :, at] / (regret_v[1, j, :, at] + regret_v[0, j, :, at])
            else:
                at = pl.ds(128 * t, LAST)
                pad[j, :, :LAST] = regret_v[1, j, :, at] / (regret_v[1, j, :, at] + regret_v[0, j, :, at])
                tile = pad[j]
            first = (j % 2 * 2 + j // 2) * NODES * UNIT
            asend[pl.ds(first + t, NODES, stride=UNIT), :] = tile
    for copy in loads:
        copy.wait()

    alive = []
    board_bits = []
    for jj in range(2):
        j = 2 * core + jj
        alive.append(jnp.where(live_s[j] > 0, 1.0, 0.0).astype(jnp.float32))
        low = jnp.int32(0)
        high = jnp.int32(0)
        for i in range(5):
            card = cards_s[j, i]
            bit = lax.shift_left(jnp.int32(1), card % 32)
            low = low | jnp.where(card < 32, bit, 0)
            high = high | jnp.where(card < 32, 0, bit)
        board_bits.append((low, high))
    inside = (scan_v[0] & scan_v[1]) != -1
    mask = [
        jnp.where(((scan_v[0] & low) | (scan_v[1] & high)) == 0, 1.0, 0.0).astype(jnp.float32)
        for low, high in board_bits
    ]

    for which, ref in enumerate((root_v, front_v)):
        for p in range(2):
            base = (2 * which + p) * NODES * UNIT
            pad[p, :, :] = jnp.zeros((NODES, 128), jnp.float32)
            pad[p, :, :LAST] = ref[p, :, pl.ds(128 * (TILES - 1), LAST)]
            for t in range(TILES):
                tile = ref[p, :, pl.ds(128 * t, 128)] if t < TILES - 1 else pad[p]
                ends[pl.ds(base + t, NODES, stride=UNIT), :] = tile

    def end_of(index, jj):
        return unit(ends, index * NODES + node)[...] * mask[jj]

    bitrow[...] = jnp.zeros(bitrow.shape, jnp.int32)
    bitrow[0:2, :] = bits_v[...]
    rankrow[...] = jnp.zeros(rankrow.shape, jnp.float32)
    for jj in range(2):
        rankrow[jj : jj + 1, :H] = rank_v[pl.ds(2 * core + jj, 1), :].astype(jnp.float32)
    for r in range(2):
        bitwide[r] = jnp.broadcast_to(bitrow[r : r + 1, :], (8, HP))
        rankwide[r] = jnp.broadcast_to(rankrow[r : r + 1, :], (8, HP))
    for t in range(TILES):
        lanes = slice(128 * t, 128 * (t + 1))
        bitcol[lanes, :] = bitrow[:, lanes].T
        rankcol[lanes, :] = rankrow[:, lanes].T

    def payoff_rows(block, _):
        at = [pl.multiple_of(block * BLOCK + 16 * i, 16) for i in range(BLOCK // 16)]
        wide = [
            [jnp.broadcast_to(ref[pl.ds(a, 16), r : r + 1], (16, 128)) for ref in (bitcol, rankcol) for r in range(2)]
            for a in at
        ]
        one = jnp.bfloat16(1)
        for t in range(TILES):
            lanes = slice(128 * t, 128 * (t + 1))
            low, high, rank0, rank1 = (
                jnp.concatenate([ref[r, :, lanes]] * 2, axis=0) for ref in (bitwide, rankwide) for r in range(2)
            )
            for a, (low_g, high_g, rank0_g, rank1_g) in zip(at, wide):
                shared = (low_g & low) | (high_g & high)
                free = jnp.where(shared == 0, 1.0, 0.0).astype(jnp.bfloat16)
                for jj, step in enumerate((rank0 - rank0_g, rank1 - rank1_g)):
                    step = step.astype(jnp.bfloat16)
                    w[jj, pl.ds(a, 16), lanes] = jnp.minimum(jnp.maximum(step, -one), one) * free
        return 0

    lax.fori_loop(0, AHEAD, payoff_rows, 0)
    pl.semaphore_wait(barrier, SECTIONS - 1 + 2 * (COLUMNS - 1))

    def a_unit(jj, to):
        return (2 * jj + to % 2) * NODES + to // 2

    def a_copy(jj, to):
        return remote(
            unit(asend, a_unit(jj, to)), unit(arecv, jj * SECTIONS + me), a_ss, a_rs.at[jj], to, col
        )

    for jj in range(2):
        for d in ORDER:
            a_copy(jj, (me + d) % SECTIONS).start()
    for jj in range(2):
        unit(arecv, jj * SECTIONS + me)[...] = unit(asend, a_unit(jj, me))[...]

    lax.fori_loop(AHEAD, HP // BLOCK, payoff_rows, 0)

    for jj in range(2):
        wait_rows(arecv, (SECTIONS - 1) * TILES, a_rs.at[jj])
        reach = [end_of(0, jj), end_of(1, jj)]
        for s in range(SECTIONS):
            go = jnp.where(inside, unit(arecv, jj * SECTIONS + s)[...], 0.5)
            q = s % 2
            unit(lsc, (2 * jj + q) * SECTIONS + s)[...] = reach[q] * (1.0 - go)
            unit(lsc, (2 * jj + 1 - q) * SECTIONS + s)[...] = reach[1 - q]
            reach[q] = reach[q] * go
        for p in range(2):
            for t in range(TILES):
                tile = lsc[pl.ds((2 * jj + p) * SECTIONS * UNIT + t, SECTIONS, stride=UNIT), :]
                lhs[jj, p * SECTIONS : (p + 1) * SECTIONS, 128 * t : 128 * (t + 1)] = tile.astype(jnp.bfloat16)
        leaf = jnp.dot(lhs[jj], w[jj], preferred_element_type=jnp.float32)
        for p in range(2):
            for t in range(TILES):
                tile = leaf[p * SECTIONS : (p + 1) * SECTIONS, 128 * t : 128 * (t + 1)]
                leafsc[pl.ds((2 * jj + 1 - p) * SECTIONS * UNIT + t, SECTIONS, stride=UNIT), :] = tile
        value = [end_of(2, jj), end_of(3, jj)]
        for s in reversed(range(SECTIONS)):
            q = s % 2
            go = jnp.where(inside, unit(arecv, jj * SECTIONS + s)[...], 0.5)
            leaf_q = unit(leafsc, (2 * jj + q) * SECTIONS + s)[...] * mask[jj]
            leaf_o = unit(leafsc, (2 * jj + 1 - q) * SECTIONS + s)[...] * mask[jj]
            gsend[s * UNIT + jj * TILES : s * UNIT + (jj + 1) * TILES, :] = leaf_q - value[q]
            value[q] = (1.0 - go) * leaf_q + go * value[q]
            value[1 - q] = leaf_o + value[1 - q]
            for p in range(2):
                row = unit(rsend, 2 * s + p, HALF)
                part = jnp.where(inside, value[p], 1.0) * alive[jj]
                row[...] = part if jj == 0 else row[...] + part

    mine = (col + 7 * me) % SECTIONS

    def r_copy(s, p):
        to = 2 * node + p
        return remote(
            unit(rsend, 2 * s + p, HALF), unit(rrecv, core * COLUMNS + col, HALF), r_ss, r_rs,
            to, (s + (SECTIONS - 7) * to) % COLUMNS,
        )

    for s in EARLY_SECTIONS:
        for p in range(2):
            @pl.when(jnp.logical_or(core != p, mine != s))
            def _(s=s, p=p):
                r_copy(s, p).start()

    unit(rrecv, core * COLUMNS + col, HALF)[...] = unit(rsend, 2 * mine + core, HALF)[...]

    def block(ref, index):
        return ref.at[pl.ds(pl.multiple_of(index * UNIT, 8), 2 * TILES), :]

    def place(to):
        return to % 2 * NODES + to // 2

    def g_copy(to):
        return remote(block(gsend, to), block(grecv, place(me)), g_ss, g_rs, to, col)

    for d in ORDER:
        g_copy((me + d) % SECTIONS).start()
    block(grecv, place(me))[...] = block(gsend, me)[...]

    wait_rows(rrecv, (2 * COLUMNS - 1) * TILES, r_rs)
    sums = [unit(rrecv, k, HALF)[...] for k in range(4)]
    for k in range(4, 2 * COLUMNS):
        sums[k % 4] = sums[k % 4] + unit(rrecv, k, HALF)[...]
    total = (sums[0] + sums[1]) + (sums[2] + sums[3])
    fsend[:TILES, :] = total / total[TILES - 1 : TILES, 127:128]

    def f_copy(to_col):
        return remote(unit(fsend, 0), unit(frecv, me), f_ss, f_rs, mine, to_col)

    for to_col in EARLY_COLUMNS:
        @pl.when(jnp.logical_or(mine != me, col != to_col))
        def _(to_col=to_col):
            f_copy(to_col).start()

    @pl.when(mine == me)
    def _():
        unit(frecv, me)[...] = fsend[:TILES, :]

    wait_rows(grecv, (SECTIONS - 1) * 2 * TILES, g_rs)
    for j in range(BOARD_DEV):
        keep = live_s[j] > 0
        for t in range(TILES):
            size = 128 if t < TILES - 1 else LAST
            at = pl.ds(128 * t, size)
            first = j // 2 * NODES * UNIT + j % 2 * TILES
            gap = grecv[pl.ds(first + t, NODES, stride=UNIT), :][:, :size]
            stop = regret_v[0, j, :, at]
            go = regret_v[1, j, :, at]
            total_regret = stop + go
            out_stop[j, :, at] = jnp.where(keep, jnp.maximum(stop + go / total_regret * gap, 0.0), stop)
            out_go[j, :, at] = jnp.where(keep, jnp.maximum(go - stop / total_regret * gap, 0.0), go)

    wait_rows(asend, (SECTIONS - 1) * 2 * TILES, a_ss)
    wait_rows(gsend, (SECTIONS - 1) * 2 * TILES, g_ss)
    wait_rows(rsend, (2 * COLUMNS - 1) * TILES, r_ss)

    @pl.when(mine != me)
    def _():
        wait_rows(frecv, COLUMNS * TILES, f_ss)

    @pl.when(mine == me)
    def _():
        wait_rows(frecv, (COLUMNS - 1) * TILES, f_ss)

    @pl.when(mine != me)
    def _():
        wait_rows(frecv, SECTIONS * TILES, f_rs)

    @pl.when(mine == me)
    def _():
        wait_rows(frecv, (SECTIONS - 1) * TILES, f_rs)

    for p in range(2):
        for t in range(TILES):
            size = 128 if t < TILES - 1 else LAST
            tile = frecv[pl.ds(p * UNIT + t, NODES, stride=2 * UNIT), :]
            out_sec[p, :, pl.ds(128 * t, size)] = tile[:, :size]


def store(stop_v, go_v, sec_v, out_stop, out_go, out_sec, sem):
    pairs = ((stop_v, out_stop), (go_v, out_go), (sec_v, out_sec))
    copies = [pltpu.make_async_copy(src, dst.at[0], sem.at[i]) for i, (src, dst) in enumerate(pairs)]
    for copy in copies:
        copy.start()
    for copy in copies:
        copy.wait()


def local(root_reach, frontier_value, regret_stop, regret_go, board_live, board_cards, hand_rank):
    bits, scan = hand_bits()
    f32, i32 = jnp.float32, jnp.int32
    regrets = (BOARD_DEV, NODES, H)
    ends = (2, NODES, H)
    hbm_spec = pl.BlockSpec(memory_space=pltpu.HBM)
    vmem_spec = pl.BlockSpec(memory_space=pltpu.VMEM)
    dma = pltpu.SemaphoreType.DMA
    operands = (
        root_reach, frontier_value, regret_stop[0], regret_go[0], board_live, board_cards, hand_rank,
        jnp.asarray(bits), jnp.asarray(scan),
    )
    new_stop, new_go, section_value = pl.pallas_call(
        kernel,
        out_shape=(
            pltpu.VMEM(regrets, f32),
            pltpu.VMEM(regrets, f32),
            pltpu.VMEM(ends, f32),
        ),
        in_specs=[hbm_spec] * 9,
        out_specs=(vmem_spec,) * 3,
        scratch_shapes=[
            pltpu.VMEM(ends, f32), pltpu.VMEM(ends, f32), pltpu.VMEM((2, *regrets), f32),
            pltpu.SMEM((BOARD_DEV,), i32), pltpu.SMEM((BOARD_DEV, 5), i32), pltpu.VMEM((BOARD_DEV, H), i32),
            pltpu.VMEM((2, HP), i32), pltpu.VMEM((2, TILES, 128), i32),
            pltpu.VMEM((BOARD_DEV, NODES, 128), f32),
            pltpu.VMEM((2 * SECTIONS * UNIT, 128), f32), pltpu.VMEM((2 * SECTIONS * UNIT, 128), f32),
            pltpu.VMEM((4 * NODES * UNIT, 128), f32),
            pltpu.VMEM((8, HP), i32), pltpu.VMEM((8, HP), f32), pltpu.VMEM((2, 8, HP), i32), pltpu.VMEM((2, 8, HP), f32),
            pltpu.VMEM((HP, 8), i32), pltpu.VMEM((HP, 8), f32),
            pltpu.VMEM((2, HP, HP), jnp.bfloat16),
            pltpu.VMEM((4 * SECTIONS * UNIT, 128), f32), pltpu.VMEM((2, 2 * SECTIONS, HP), jnp.bfloat16),
            pltpu.VMEM((4 * SECTIONS * UNIT, 128), f32),
            pltpu.VMEM((SECTIONS * UNIT, 128), f32), pltpu.VMEM((SECTIONS * UNIT, 128), f32),
            pltpu.VMEM((2 * SECTIONS * HALF, 128), f32), pltpu.VMEM((2 * COLUMNS * HALF, 128), f32),
            pltpu.VMEM((HALF, 128), f32), pltpu.VMEM((SECTIONS * UNIT, 128), f32),
            dma((7,)), dma, dma, dma((2,)), *([dma] * 6),
        ],
        compiler_params=pltpu.CompilerParams(
            collective_id=0, has_side_effects=True, vmem_limit_bytes=32 * 1024 * 1024
        ),
    )(*(pltpu.with_memory_space_constraint(x, pltpu.HBM) for x in operands))
    return pl.pallas_call(
        store,
        out_shape=(
            jax.ShapeDtypeStruct((1, *regrets), f32),
            jax.ShapeDtypeStruct((1, *regrets), f32),
            jax.ShapeDtypeStruct((1, *ends), f32),
        ),
        in_specs=[vmem_spec] * 3,
        out_specs=(hbm_spec,) * 3,
        scratch_shapes=[dma((3,))],
        compiler_params=pltpu.CompilerParams(vmem_limit_bytes=1024 * 1024),
    )(new_stop, new_go, section_value)


def solution(mesh):
    regrets = P("section", "board", None, None)
    return jax.shard_map(
        local,
        mesh=mesh,
        in_specs=(P(), P(), regrets, regrets, P("board"), P("board", None), P("board", None)),
        out_specs=(regrets, regrets, P("section", None, None, None)),
        check_vma=False,
    )
```
